128 devices in a mesh: tp: 16 (over z, y), dp: 8 (over x, core).
Axes of the slice: x: 4, y: 4, z: 4, core: 2. Of those that a mesh axis runs over, the one named last changes fastest.
Arguments:
- x_in: bfloat16 [2048, 4096], P(('dp', 'tp'))
- w_gate: bfloat16 [4096, 16384], P('dp', 'tp')
- w_up: bfloat16 [4096, 16384], P('dp', 'tp')
- w_down: bfloat16 [16384, 4096], P('tp', 'dp')
- grad_y: bfloat16 [2048, 4096], P(('dp', 'tp'))
Outputs:
- output 1: bfloat16 [2048, 4096], P(('dp', 'tp'))
- output 2: bfloat16 [2048, 4096], P(('dp', 'tp'))
- output 3: float32 [4096, 16384], P('dp', 'tp')
- output 4: float32 [4096, 16384], P('dp', 'tp')
- output 5: float32 [16384, 4096], P('tp', 'dp')
All inputs are finite; a program needn't handle non-finite values.
Results may differ from the reference program's by a relative error of at most 0.00141.
Values are sent between devices in bfloat16 or wider.
A program may use at most 1 GiB of HBM per device.

```python
import jax
import jax.numpy as jnp

D = 4096
FF = 16384
TOKENS = 2048


def setup_inputs(seed: int = 0) -> dict:
    base_key = jax.random.key(seed)
    key_list = jax.random.split(base_key, 5)
    x_in = jax.random.normal(key_list[0], (TOKENS, D), jnp.float32).astype(jnp.bfloat16)
    w_gate = (jax.random.normal(key_list[1], (D, FF), jnp.float32) * D ** -0.5).astype(jnp.bfloat16)
    w_up = (jax.random.normal(key_list[2], (D, FF), jnp.float32) * D ** -0.5).astype(jnp.bfloat16)
    w_down = (jax.random.normal(key_list[3], (FF, D), jnp.float32) * FF ** -0.5).astype(jnp.bfloat16)
    grad_y = jax.random.normal(key_list[4], (TOKENS, D), jnp.float32).astype(jnp.bfloat16)
    return {"x_in": x_in, "w_gate": w_gate, "w_up": w_up, "w_down": w_down, "grad_y": grad_y}


def reference(x_in, w_gate, w_up, w_down, grad_y):
    gate_pre = jnp.dot(x_in, w_gate, preferred_element_type=jnp.float32)
    up_pre = jnp.dot(x_in, w_up, preferred_element_type=jnp.float32)
    sig_gate = jax.nn.sigmoid(gate_pre)
    silu_gate = gate_pre * sig_gate
    hidden = (silu_gate * up_pre).astype(jnp.bfloat16)
    y_out = (x_in.astype(jnp.float32) + jnp.dot(hidden, w_down, preferred_element_type=jnp.float32)).astype(jnp.bfloat16)
    grad_h = jnp.dot(grad_y, w_down.T, preferred_element_type=jnp.float32)
    silu_deriv = sig_gate * (1.0 + gate_pre * (1.0 - sig_gate))
    grad_gate = (grad_h * up_pre * silu_deriv).astype(jnp.bfloat16)
    grad_up = (grad_h * silu_gate).astype(jnp.bfloat16)
    grad_x = (grad_y.astype(jnp.float32)
              + jnp.dot(grad_gate, w_gate.T, preferred_element_type=jnp.float32)
              + jnp.dot(grad_up, w_up.T, preferred_element_type=jnp.float32)).astype(jnp.bfloat16)
    grad_w_gate = jnp.dot(x_in.T, grad_gate, preferred_element_type=jnp.float32)
    grad_w_up = jnp.dot(x_in.T, grad_up, preferred_element_type=jnp.float32)
    grad_w_down = jnp.dot(hidden.T, grad_y, preferred_element_type=jnp.float32)
    return (y_out, grad_x, grad_w_gate, grad_w_up, grad_w_down)
```

```python
import jax
import jax.numpy as jnp
from jax import lax
from jax.experimental import pallas as pl
from jax.experimental.pallas import tpu as pltpu
from jax.sharding import PartitionSpec as P

RING = 4
N_DP = 2 * RING
VMEM = pltpu.MemorySpace.VMEM


class Links:
    def __init__(self, send_sem, recv_sem, local_sem):
        self.send_sem, self.recv_sem, self.local_sem = send_sem, recv_sem, local_sem
        self.n_remote = self.n_local = 0
        self.sent, self.local = [], []
        dp, tp = lax.axis_index("dp"), lax.axis_index("tp")
        self.dp, self.tp = dp, tp
        self.x, self.core = dp // 2, dp % 2
        self.z, self.y = tp // RING, tp % RING

    def at(self, pos, off):
        return (pos + off) % RING

    def device(self, axis, off):
        if axis == "x":
            return {"dp": 2 * self.at(self.x, off) + self.core, "tp": self.tp}
        if axis == "core":
            return {"dp": 2 * self.x + (1 - self.core), "tp": self.tp}
        if axis == "dp":
            return {"dp": (self.dp + off) % N_DP, "tp": self.tp}
        if axis == "z":
            return {"dp": self.dp, "tp": RING * self.at(self.z, off) + self.y}
        return {"dp": self.dp, "tp": RING * self.z + self.at(self.y, off)}

    def barrier(self, peers):
        sem = pltpu.get_barrier_semaphore()
        for axis, off in peers:
            pl.semaphore_signal(sem, inc=1, device_id=self.device(axis, off),
                                device_id_type=pl.DeviceIdType.MESH)
        pl.semaphore_wait(sem, len(peers))

    def send(self, src, dst, axis, off=0):
        k = self.n_remote
        self.n_remote += 1
        copy = pltpu.make_async_remote_copy(
            src_ref=src, dst_ref=dst, send_sem=self.send_sem.at[k], recv_sem=self.recv_sem.at[k],
            device_id=self.device(axis, off), device_id_type=pl.DeviceIdType.MESH)
        copy.start()
        self.sent.append(copy)
        return copy

    def put(self, src, dst):
        k = self.n_local
        self.n_local += 1
        copy = pltpu.make_async_copy(src, dst, self.local_sem.at[k])
        copy.start()
        self.local.append(copy)
        return copy

    def finish(self, waited=()):
        for copy in self.sent:
            copy.wait_send()
        for copy in self.local:
            if not any(copy is w for w in waited):
                copy.wait()


def gather_start(links, own, block, axis, pos):
    right = links.send(own, block(pos, None), axis, 1)
    left = links.send(own, block(pos, None), axis, -1)
    return right, left


def gather_forward(links, copies, block, axis, pos):
    copies[0].wait_recv()
    from_left = links.at(pos, -1)
    right = links.send(block(from_left, 0), block(from_left, 0), axis, 1)
    copies[1].wait_recv()
    from_right = links.at(pos, 1)
    left = links.send(block(from_right, 1), block(from_right, 1), axis, -1)
    return right, left


def gather_end(copies):
    for copy in copies:
        copy.wait_recv()


def dp_gather_start(links, own, slot):
    x, c = links.x, links.core
    block = lambda p, h: slot(2 * p + c, h)
    copies = gather_start(links, own, block, "x", x)
    mate = [links.send(own, slot(links.dp, None), "core")]
    return block, copies, mate


def dp_gather_forward(links, state):
    block, copies, mate = state
    x = links.x
    onward = gather_forward(links, copies, block, "x", x)
    for off in (-1, 1):
        b = block(links.at(x, off), None)
        mate.append(links.send(b, b, "core"))
    return block, onward, mate


def dp_gather_end(links, state):
    block, onward, mate = state
    far = links.at(links.x, 2)
    for h in (0, 1):
        onward[h].wait_recv()
        mate.append(links.send(block(far, h), block(far, h), "core"))
    return mate


def gather_kernel(x_ref, gy_ref, wg_ref, wu_ref, wd_ref,
                  xr_ref, gr_ref, xc_ref, gc_ref, wgf_ref, wuf_ref, wdf_ref,
                  send_sem, recv_sem, local_sem):
    links = Links(send_sem, recv_sem, local_sem)
    dp, z, y = links.dp, links.z, links.y
    links.barrier([("dp", o) for o in range(1, N_DP)] + [("z", 1), ("z", -1), ("y", 1), ("y", -1)])

    d_loc = wg_ref.shape[0]
    half_cols = x_ref.shape[1] // 2

    def row_slot(w_ref):
        rows = wg_ref.shape[0]

        def slot(j, h):
            if h is None:
                return w_ref.at[pl.ds(pl.multiple_of(j * rows, rows), rows)]
            return w_ref.at[pl.ds(pl.multiple_of(j * rows + h * (rows // 2), rows // 2), rows // 2)]
        return slot

    def col_slot(j, h):
        cols = pl.ds(pl.multiple_of(j * d_loc, d_loc), d_loc)
        rows = wd_ref.shape[0]
        if h is None:
            return wdf_ref.at[:, cols]
        return wdf_ref.at[pl.ds(h * (rows // 2), rows // 2), cols]

    def d_slice(ref, j):
        return ref.at[:, pl.ds(pl.multiple_of(j * d_loc, d_loc), d_loc)]

    def spread(src, dst):
        copies = [links.send(d_slice(src, (dp + o) % N_DP), dst.at[dp, z, y], "dp", o) for o in range(1, N_DP)]
        return copies, links.put(d_slice(src, dp), dst.at[dp, z, y])

    spread_x = spread(x_ref, xc_ref)
    spread_g = spread(gy_ref, gc_ref)

    def half(h):
        return pl.ds(h * half_cols, half_cols)

    def xr_first(p, h):
        return xr_ref.at[p, y] if h is None else xr_ref.at[p, y, :, half(h)]

    def xr_second(p, h):
        return xr_ref.at[:, p] if h is None else xr_ref.at[pl.ds(2 * h, 2), p]

    def gr_first(p, h):
        return gr_ref.at[z, p] if h is None else gr_ref.at[z, p, :, half(h)]

    def gr_second(p, h):
        return gr_ref.at[p] if h is None else gr_ref.at[p, pl.ds(2 * h, 2)]

    def dp_half(h):
        return pl.ds(h * (N_DP // 2), N_DP // 2)

    def xc_first(p, h):
        return xc_ref.at[:, p, y] if h is None else xc_ref.at[dp_half(h), p, y]

    def xc_second(p, h):
        return xc_ref.at[:, :, p] if h is None else xc_ref.at[dp_half(h), :, p]

    def gc_first(p, h):
        return gc_ref.at[:, z, p] if h is None else gc_ref.at[dp_half(h), z, p]

    def gc_second(p, h):
        return gc_ref.at[:, p] if h is None else gc_ref.at[dp_half(h), p]

    own_rows = [links.put(x_ref, xr_ref.at[z, y]), links.put(gy_ref, gr_ref.at[z, y])]
    xr = gather_start(links, x_ref, xr_first, "z", z)
    gr = gather_start(links, gy_ref, gr_first, "y", y)

    weights = [dp_gather_start(links, wg_ref, row_slot(wgf_ref)),
               dp_gather_start(links, wu_ref, row_slot(wuf_ref)),
               dp_gather_start(links, wd_ref, col_slot)]
    links.put(wg_ref, row_slot(wgf_ref)(dp, None))
    links.put(wu_ref, row_slot(wuf_ref)(dp, None))
    links.put(wd_ref, col_slot(dp, None))

    for copies, own in (spread_x, spread_g):
        for copy in copies:
            copy.wait_recv()
        own.wait()
    xc = gather_start(links, xc_first(z, None), xc_first, "z", z)
    gc = gather_start(links, gc_first(y, None), gc_first, "y", y)

    xr = gather_forward(links, xr, xr_first, "z", z)
    gr = gather_forward(links, gr, gr_first, "y", y)
    xc = gather_forward(links, xc, xc_first, "z", z)
    gc = gather_forward(links, gc, gc_first, "y", y)

    for copy in own_rows:
        copy.wait()
    gather_end(xr)
    xr = gather_start(links, xr_second(y, None), xr_second, "y", y)
    gather_end(gr)
    gr = gather_start(links, gr_second(z, None), gr_second, "z", z)
    gather_end(xc)
    xc = gather_start(links, xc_second(y, None), xc_second, "y", y)
    gather_end(gc)
    gc = gather_start(links, gc_second(z, None), gc_second, "z", z)

    weights[0] = dp_gather_forward(links, weights[0])
    xr = gather_forward(links, xr, xr_second, "y", y)
    gr = gather_forward(links, gr, gr_second, "z", z)
    xc = gather_forward(links, xc, xc_second, "y", y)
    gc = gather_forward(links, gc, gc_second, "z", z)
    weights[1] = dp_gather_forward(links, weights[1])
    weights[2] = dp_gather_forward(links, weights[2])

    for copies in (xr, gr, xc, gc):
        gather_end(copies)
    mates = [dp_gather_end(links, w) for w in weights]
    for mate in mates:
        gather_end(mate)
    links.finish(waited=[spread_x[1], spread_g[1]] + own_rows)


CHUNK = 1024


def add_into(dst, terms, write=None):
    lead, (rows, cols) = dst.shape[:-2], dst.shape[-2:]
    step = min(CHUNK, cols)
    for i in range(lead[0] if lead else 1):
        for c in range(0, cols, step):
            idx = ((i,) if lead else ()) + (slice(None), slice(c, c + step))
            total = terms[0][idx]
            for t in terms[1:]:
                total = total + t[idx]
            dst[idx] = total


def scatter_start(links, block, bufs, axis, pos):
    near0, near1, l_ref, r_ref, _, _ = bufs
    far = links.at(pos, 2)
    to_right = links.send(block(far, 0), near0, axis, 1)
    to_left = links.send(block(far, 1), near1, axis, -1)
    plain_r = links.send(block(links.at(pos, 1), 1), l_ref.at[1], axis, 1)
    plain_l = links.send(block(links.at(pos, -1), 0), r_ref.at[0], axis, -1)
    return to_right, to_left, plain_r, plain_l


def scatter_forward(links, state, block, bufs, axis, pos):
    near0, near1, l_ref, r_ref, stage_r, stage_l = bufs
    to_right, to_left, plain_r, plain_l = state
    to_right.wait_recv()
    add_into(stage_r, [block(links.at(pos, 1), 0), near0])
    sum_r = links.send(stage_r, l_ref.at[0], axis, 1)
    to_left.wait_recv()
    add_into(stage_l, [block(links.at(pos, -1), 1), near1])
    sum_l = links.send(stage_l, r_ref.at[1], axis, -1)
    return plain_r, plain_l, sum_r, sum_l


def exchange_kernel(h_ref, da_ref, db_ref, yp_ref, gp_ref, x_ref, gy_ref,
                    ha_ref, daa_ref, dba_ref, y_ref, gx_ref,
                    yn0, yn1, yl, yr, ysr, ysl, yres,
                    gn0, gn1, gl, gr, gsr, gsl, gres,
                    yn0b, yn1b, ylb, yrb, ysrb, yslb,
                    gn0b, gn1b, glb, grb, gsrb, gslb,
                    send_sem, recv_sem, local_sem):
    links = Links(send_sem, recv_sem, local_sem)
    dp, z, y = links.dp, links.z, links.y
    links.barrier([("x", 1), ("x", -1), ("core", 0), ("z", 1), ("z", -1), ("y", 1), ("y", -1)])

    rows = h_ref.shape[0]

    def row_slot(ref):
        def slot(j, h):
            if h is None:
                return ref.at[pl.ds(pl.multiple_of(j * rows, rows), rows)]
            return ref.at[pl.ds(pl.multiple_of(j * rows + h * (rows // 2), rows // 2), rows // 2)]
        return slot

    def y_first(p, h):
        return yp_ref.at[p, pl.ds(2 * h, 2)]

    def g_first(p, h):
        return gp_ref.at[pl.ds(2 * h, 2), p]

    half_cols = x_ref.shape[1] // 2

    def y_second(p, h):
        return yres.at[p, :, pl.ds(h * half_cols, half_cols)]

    def g_second(p, h):
        return gres.at[p, :, pl.ds(h * half_cols, half_cols)]

    yb1, gb1 = (yn0, yn1, yl, yr, ysr, ysl), (gn0, gn1, gl, gr, gsr, gsl)
    yb2, gb2 = (yn0b, yn1b, ylb, yrb, ysrb, yslb), (gn0b, gn1b, glb, grb, gsrb, gslb)

    ys = scatter_start(links, y_first, yb1, "z", z)
    gs = scatter_start(links, g_first, gb1, "y", y)
    refs = ((h_ref, ha_ref), (da_ref, daa_ref), (db_ref, dba_ref))
    acts = [dp_gather_start(links, src, row_slot(dst)) for src, dst in refs]
    for src, dst in refs:
        links.put(src, row_slot(dst)(dp, None))

    ys = scatter_forward(links, ys, y_first, yb1, "z", z)
    gs = scatter_forward(links, gs, g_first, gb1, "y", y)
    for i in range(3):
        acts[i] = dp_gather_forward(links, acts[i])

    gather_end(ys)
    for h in (0, 1):
        add_into(yres.at[pl.ds(2 * h, 2)], [y_first(z, h), yl.at[h], yr.at[h]])
    ys = scatter_start(links, y_second, yb2, "y", y)
    gather_end(gs)
    for h in (0, 1):
        add_into(gres.at[pl.ds(2 * h, 2)], [g_first(y, h), gl.at[h], gr.at[h]])
    gs = scatter_start(links, g_second, gb2, "z", z)
    ys = scatter_forward(links, ys, y_second, yb2, "y", y)
    gs = scatter_forward(links, gs, g_second, gb2, "z", z)

    mates = [dp_gather_end(links, acts[0])]
    gather_end(ys)
    gather_end(gs)
    step = min(CHUNK, half_cols)
    for own, second, pos, l_ref, r_ref, resid, out in (
            (yres, y_second, y, ylb, yrb, x_ref, y_ref), (gres, g_second, z, glb, grb, gy_ref, gx_ref)):
        for h in (0, 1):
            for c in range(0, half_cols, step):
                part = slice(c, c + step)
                both = slice(h * half_cols + c, h * half_cols + c + step)
                total = second(pos, h)[:, part] + l_ref[h, :, part] + r_ref[h, :, part]
                out[:, both] = (resid[:, both].astype(jnp.float32) + total).astype(out.dtype)

    mates += [dp_gather_end(links, acts[1]), dp_gather_end(links, acts[2])]
    for mate in mates:
        gather_end(mate)
    links.finish()


def solution(mesh):
    vmem = pl.BlockSpec(memory_space=VMEM)
    hbm = pl.BlockSpec(memory_space=pl.ANY)

    def local_step(x_loc, wg_loc, wu_loc, wd_loc, gy_loc):
        tok, d = x_loc.shape
        d_loc, ff = wg_loc.shape
        bf16, f32 = x_loc.dtype, jnp.float32
        sds = jax.ShapeDtypeStruct
        n_sem = 80
        xr, gr, xc, gc, wg, wu, wd = pl.pallas_call(
            gather_kernel,
            out_shape=[sds((RING, RING, tok, d), bf16), sds((RING, RING, tok, d), bf16),
                       sds((N_DP, RING, RING, tok, d_loc), bf16), sds((N_DP, RING, RING, tok, d_loc), bf16),
                       sds((d, ff), bf16), sds((d, ff), bf16), sds((ff, d), bf16)],
            in_specs=[vmem] * 5,
            out_specs=[hbm] * 7,
            scratch_shapes=[pltpu.SemaphoreType.DMA((n_sem,)), pltpu.SemaphoreType.DMA((n_sem,)),
                            pltpu.SemaphoreType.DMA((8,))],
            compiler_params=pltpu.CompilerParams(collective_id=0, has_side_effects=True),
            name="gather_all",
        )(x_loc, gy_loc, wg_loc, wu_loc, wd_loc)
        rows = RING * RING * tok
        x_rows, gy_rows = xr.reshape(rows, d), gr.reshape(rows, d)
        x_cols, gy_cols = xc.reshape(N_DP * rows, d_loc), gc.reshape(N_DP * rows, d_loc)

        gate_pre = jnp.dot(x_rows, wg, preferred_element_type=f32)
        up_pre = jnp.dot(x_rows, wu, preferred_element_type=f32)
        grad_h = jnp.einsum("nd,fd->nf", gy_rows, wd, preferred_element_type=f32)
        sig_gate = jax.nn.sigmoid(gate_pre)
        silu_gate = gate_pre * sig_gate
        hidden = (silu_gate * up_pre).astype(bf16)
        silu_deriv = sig_gate * (1.0 + gate_pre * (1.0 - sig_gate))
        grad_gate = (grad_h * up_pre * silu_deriv).astype(bf16)
        grad_up = (grad_h * silu_gate).astype(bf16)
        y_part = jnp.dot(hidden, wd, preferred_element_type=f32)
        gx_part = (jnp.einsum("nf,df->nd", grad_gate, wg, preferred_element_type=f32)
                   + jnp.einsum("nf,df->nd", grad_up, wu, preferred_element_type=f32))

        torus = (RING, RING, tok, d)
        half1, half2 = (2, tok, d), (tok, d // 2)
        first = [pltpu.VMEM(half1, f32)] * 2 + [pltpu.VMEM((2,) + half1, f32)] * 2 + [pltpu.VMEM(half1, f32)] * 2
        second = [pltpu.VMEM(half2, f32)] * 2 + [pltpu.VMEM((2,) + half2, f32)] * 2 + [pltpu.VMEM(half2, f32)] * 2
        res = [pltpu.VMEM((RING, tok, d), f32)]
        full = sds((N_DP * rows, ff), bf16)
        h_all, da_all, db_all, y_rows, gx_rows = pl.pallas_call(
            exchange_kernel,
            out_shape=[full, full, full, sds((tok, d), bf16), sds((tok, d), bf16)],
            in_specs=[vmem] * 7,
            out_specs=[hbm] * 3 + [vmem] * 2,
            scratch_shapes=first + res + first + res + second + second
            + [pltpu.SemaphoreType.DMA((n_sem,)), pltpu.SemaphoreType.DMA((n_sem,)), pltpu.SemaphoreType.DMA((8,))],
            compiler_params=pltpu.CompilerParams(collective_id=1, has_side_effects=True),
            name="exchange",
        )(hidden, grad_gate, grad_up, y_part.reshape(torus), gx_part.reshape(torus), x_loc, gy_loc)

        grad_wd = jnp.einsum("nf,nd->fd", h_all, gy_cols, preferred_element_type=f32)
        grad_wg = jnp.einsum("nd,nf->df", x_cols, da_all, preferred_element_type=f32)
        grad_wu = jnp.einsum("nd,nf->df", x_cols, db_all, preferred_element_type=f32)
        return y_rows, gx_rows, grad_wg, grad_wu, grad_wd

    row_spec = P(("dp", "tp"), None)
    up_spec = P("dp", "tp")
    down_spec = P("tp", "dp")
    return jax.shard_map(local_step, mesh=mesh,
                         in_specs=(row_spec, up_spec, up_spec, down_spec, row_spec),
                         out_specs=(row_spec, row_spec, up_spec, up_spec, down_spec),
                         check_vma=False)
```

```python
import jax
import jax.numpy as jnp
from jax import lax
from jax.experimental import pallas as pl
from jax.experimental.pallas import tpu as pltpu
from jax.sharding import PartitionSpec as P

RING = 4
N_DP = 2 * RING
VMEM = pltpu.MemorySpace.VMEM


class Links:
    def __init__(self, send_sem, recv_sem, local_sem):
        self.send_sem, self.recv_sem, self.local_sem = send_sem, recv_sem, local_sem
        self.n_remote = self.n_local = 0
        self.sent, self.local = [], []
        dp, tp = lax.axis_index("dp"), lax.axis_index("tp")
        self.dp, self.tp = dp, tp
        self.x, self.core = dp // 2, dp % 2
        self.z, self.y = tp // RING, tp % RING

    def at(self, pos, off):
        return (pos + off) % RING

    def device(self, axis, off):
        if axis == "x":
            return {"dp": 2 * self.at(self.x, off) + self.core, "tp": self.tp}
        if axis == "core":
            return {"dp": 2 * self.x + (1 - self.core), "tp": self.tp}
        if axis == "dp":
            return {"dp": (self.dp + off) % N_DP, "tp": self.tp}
        if axis == "z":
            return {"dp": self.dp, "tp": RING * self.at(self.z, off) + self.y}
        return {"dp": self.dp, "tp": RING * self.z + self.at(self.y, off)}

    def barrier(self, peers):
        sem = pltpu.get_barrier_semaphore()
        for axis, off in peers:
            pl.semaphore_signal(sem, inc=1, device_id=self.device(axis, off),
                                device_id_type=pl.DeviceIdType.MESH)
        pl.semaphore_wait(sem, len(peers))

    def send(self, src, dst, axis, off=0):
        k = self.n_remote
        self.n_remote += 1
        copy = pltpu.make_async_remote_copy(
            src_ref=src, dst_ref=dst, send_sem=self.send_sem.at[k], recv_sem=self.recv_sem.at[k],
            device_id=self.device(axis, off), device_id_type=pl.DeviceIdType.MESH)
        copy.start()
        self.sent.append(copy)
        return copy

    def put(self, src, dst):
        k = self.n_local
        self.n_local += 1
        copy = pltpu.make_async_copy(src, dst, self.local_sem.at[k])
        copy.start()
        self.local.append(copy)
        return copy

    def sent_all(self):
        for copy in self.sent:
            copy.wait_send()
        self.sent = []

    def put_all(self):
        for copy in self.local:
            copy.wait()
        self.local = []


def gather_start(links, own, block, axis, pos):
    right = links.send(own, block(pos, None), axis, 1)
    left = links.send(own, block(pos, None), axis, -1)
    return right, left


def gather_forward(links, copies, block, axis, pos):
    copies[0].wait_recv()
    from_left = links.at(pos, -1)
    right = links.send(block(from_left, 0), block(from_left, 0), axis, 1)
    copies[1].wait_recv()
    from_right = links.at(pos, 1)
    left = links.send(block(from_right, 1), block(from_right, 1), axis, -1)
    return right, left


def gather_end(copies):
    for copy in copies:
        copy.wait_recv()


class DpGather:
    def __init__(self, links, own, slot):
        self.links, self.slot = links, slot
        x, c = links.x, links.core
        self.block = lambda p, h: slot(2 * p + c, h)
        self.ring = gather_start(links, own, self.block, "x", x)
        self.mate = [links.send(own, slot(links.dp, None), "core")]

    def forward(self):
        links = self.links
        self.ring = gather_forward(links, self.ring, self.block, "x", links.x)
        for off in (-1, 1):
            b = self.block(links.at(links.x, off), None)
            self.mate.append(links.send(b, b, "core"))

    def near(self):
        gather_end(self.mate)
        self.mate = []

    def far(self):
        links = self.links
        far = links.at(links.x, 2)
        for h in (0, 1):
            self.ring[h].wait_recv()
            b = self.block(far, h)
            self.mate.append(links.send(b, b, "core"))


class Scatter:
    def __init__(self, links, part, cols, z_first, bufs):
        self.links, z, y = links, links.z, links.y
        lo, width = cols
        half = width // 2
        self.half = half
        both = pl.ds(lo, width)
        if z_first:
            self.axes, self.pos = ("z", "y"), (z, y)
            first = lambda p, h: part.at[p, pl.ds(2 * h, 2), :, both]
            second = lambda p, h: part.at[z, p, :, pl.ds(lo + h * half, half)]
        else:
            self.axes, self.pos = ("y", "z"), (y, z)
            first = lambda p, h: part.at[pl.ds(2 * h, 2), p, :, both]
            second = lambda p, h: part.at[p, y, :, pl.ds(lo + h * half, half)]
        self.block = (first, second)
        self.bufs = (bufs[:4], bufs[4:])

    def start(self, phase):
        links, block, axis, pos = self.links, self.block[phase], self.axes[phase], self.pos[phase]
        near0, near1, l_ref, r_ref = self.bufs[phase]
        far = links.at(pos, 2)
        self.first = (links.send(block(far, 0), near0, axis, 1), links.send(block(far, 1), near1, axis, -1))
        self.last = [links.send(block(links.at(pos, 1), 1), l_ref.at[1], axis, 1),
                     links.send(block(links.at(pos, -1), 0), r_ref.at[0], axis, -1)]

    def forward(self, phase):
        links, block, axis, pos = self.links, self.block[phase], self.axes[phase], self.pos[phase]
        near0, near1, l_ref, r_ref = self.bufs[phase]
        for copy, off, h, near, dst in ((self.first[0], 1, 0, near0, l_ref), (self.first[1], -1, 1, near1, r_ref)):
            copy.wait_recv()
            b = block(links.at(pos, off), h)
            add_into(b, [near])
            self.last.append(links.send(b, dst.at[h], axis, off))

    def end(self, phase):
        block, pos = self.block[phase], self.pos[phase]
        _, _, l_ref, r_ref = self.bufs[phase]
        gather_end(self.last)
        for h in (0, 1):
            add_into(block(pos, h), [l_ref.at[h], r_ref.at[h]])

    def result(self, h):
        return self.block[1](self.pos[1], h)


CHUNK = 1024
TILE = 256


def add_into(dst, terms):
    lead, cols = dst.shape[:-2], dst.shape[-1]
    step = min(CHUNK, cols)
    for i in range(lead[0] if lead else 1):
        for c in range(0, cols, step):
            idx = ((i,) if lead else ()) + (slice(None), slice(c, c + step))
            total = dst[idx]
            for t in terms:
                total = total + t[idx]
            dst[idx] = total


def loop(n, body):
    def step(i, carry):
        body(i)
        return carry
    lax.fori_loop(0, n, step, 0)


def part_of(i, size):
    return pl.ds(pl.multiple_of(i * size, size), size)


NN = (((1,), (0,)), ((), ()))
NT = (((1,), (1,)), ((), ()))
TN = (((0,), (0,)), ((), ()))


def dot(a, b, dims):
    return lax.dot_general(a, b, dims, preferred_element_type=jnp.float32)


def mlp_kernel(x_ref, gy_ref, wg_ref, wu_ref, wd_ref,
               y_ref, gx_ref, gwg_ref, gwu_ref, gwd_ref, xc_ref, gc_ref,
               wgf, wuf, wdf, xr, gr, ha, daa, dba, acc_g, acc_u, acc_d, y_part, gx_part, *rest):
    scat_bufs, (send_sem, recv_sem, local_sem) = rest[:-3], rest[-3:]
    links = Links(send_sem, recv_sem, local_sem)
    dp, z, y, x = links.dp, links.z, links.y, links.x
    tok, d = x_ref.shape
    d_loc, ff = wg_ref.shape
    rows = RING * RING * tok
    bf16 = x_ref.dtype
    links.barrier([("dp", o) for o in range(1, N_DP)] + [("z", 1), ("z", -1), ("y", 1), ("y", -1)])

    def row_slot(ref, n):
        def slot(j, h):
            if h is None:
                return ref.at[part_of(j, n)]
            return ref.at[part_of(2 * j + h, n // 2)]
        return slot

    def col_slot(j, h):
        if h is None:
            return wdf.at[:, part_of(j, d_loc)]
        return wdf.at[pl.ds(h * (ff // 2), ff // 2), part_of(j, d_loc)]

    def spread(src, dst):
        def d_slice(j):
            return src.at[:, part_of(j, d_loc)]
        return ([links.send(d_slice((dp + o) % N_DP), dst.at[dp, z, y], "dp", o) for o in range(1, N_DP)],
                links.put(d_slice(dp), dst.at[dp, z, y]))

    spread_x = spread(x_ref, xc_ref)
    spread_g = spread(gy_ref, gc_ref)

    def row_half(h):
        return pl.ds(h * (d // 2), d // 2)

    def dp_half(h):
        return pl.ds(h * (N_DP // 2), N_DP // 2)

    def xr_first(p, h):
        return xr.at[p, y] if h is None else xr.at[p, y, :, row_half(h)]

    def xr_second(p, h):
        return xr.at[:, p] if h is None else xr.at[pl.ds(2 * h, 2), p]

    def gr_first(p, h):
        return gr.at[z, p] if h is None else gr.at[z, p, :, row_half(h)]

    def gr_second(p, h):
        return gr.at[p] if h is None else gr.at[p, pl.ds(2 * h, 2)]

    def xc_first(p, h):
        return xc_ref.at[:, p, y] if h is None else xc_ref.at[dp_half(h), p, y]

    def xc_second(p, h):
        return xc_ref.at[:, :, p] if h is None else xc_ref.at[dp_half(h), :, p]

    def gc_first(p, h):
        return gc_ref.at[:, z, p] if h is None else gc_ref.at[dp_half(h), z, p]

    def gc_second(p, h):
        return gc_ref.at[:, p] if h is None else gc_ref.at[dp_half(h), p]

    links.put(x_ref, xr.at[z, y])
    links.put(gy_ref, gr.at[z, y])
    rx = gather_start(links, x_ref, xr_first, "z", z)
    rg = gather_start(links, gy_ref, gr_first, "y", y)

    gate = DpGather(links, wg_ref, row_slot(wgf, d_loc))
    up = DpGather(links, wu_ref, row_slot(wuf, d_loc))
    down = DpGather(links, wd_ref, col_slot)
    links.put(wg_ref, wgf.at[part_of(dp, d_loc)])
    links.put(wu_ref, wuf.at[part_of(dp, d_loc)])
    links.put(wd_ref, wdf.at[:, part_of(dp, d_loc)])

    gather_end(spread_x[0])
    gather_end(spread_g[0])
    links.put_all()
    cx = gather_start(links, xc_first(z, None), xc_first, "z", z)
    cg = gather_start(links, gc_first(y, None), gc_first, "y", y)

    rx = gather_forward(links, rx, xr_first, "z", z)
    rg = gather_forward(links, rg, gr_first, "y", y)
    cx = gather_forward(links, cx, xc_first, "z", z)
    cg = gather_forward(links, cg, gc_first, "y", y)
    gather_end(rx)
    rx = gather_start(links, xr_second(y, None), xr_second, "y", y)
    gather_end(rg)
    rg = gather_start(links, gr_second(z, None), gr_second, "z", z)
    gather_end(cx)
    cx = gather_start(links, xc_second(y, None), xc_second, "y", y)
    gather_end(cg)
    cg = gather_start(links, gc_second(z, None), gc_second, "z", z)
    gate.forward()
    rx = gather_forward(links, rx, xr_second, "y", y)
    rg = gather_forward(links, rg, gr_second, "z", z)
    cx = gather_forward(links, cx, xc_second, "y", y)
    cg = gather_forward(links, cg, gc_second, "z", z)
    for copies in (rx, rg, cx, cg):
        gather_end(copies)

    a_acc, b_acc, g_acc = acc_g.at[pl.ds(0, rows)], acc_g.at[pl.ds(rows, rows)], acc_u.at[pl.ds(0, rows)]
    ff_tile = min(TILE, ff)
    n_ff = ff // ff_tile
    d_tile = min(TILE, d_loc)
    n_d = d_loc // d_tile

    def near_block(i):
        q = i // 2
        return 2 * ((x + q + q // 2) % RING) + i % 2

    def far_block(i):
        return 2 * ((x + 2) % RING) + i % 2

    def cols_of(ref, j):
        return ref[:, :, :, part_of(j, d_loc)].reshape(rows, d_loc)

    def clear(*refs):
        for ref in refs:
            n, step = ref.shape[0], min(16, ref.shape[0])

            def body(i):
                ref[part_of(i, step)] = jnp.zeros((step, ref.shape[1]), jnp.float32)
            loop(n // step, body)

    def add_up_side(acc, w, src, block, n):
        def body(i):
            j, t = block(i // n_ff), part_of(i % n_ff, ff_tile)
            acc[:, t] += dot(cols_of(src, j), w[part_of(j, d_loc), t], NN)
        loop(n * n_ff, body)

    def add_down_side(block, n):
        def body(i):
            j, t = block(i // n_ff), part_of(i % n_ff, ff_tile)
            g_acc[:, t] += dot(cols_of(gr, j), wdf[t, part_of(j, d_loc)], NT)
        loop(n * n_ff, body)

    clear(acc_g, acc_u)
    up.forward()
    gate.near()
    add_up_side(a_acc, wgf, xr, near_block, 6)
    up.near()
    add_up_side(b_acc, wuf, xr, near_block, 6)
    down.forward()
    down.near()
    add_down_side(near_block, 6)

    gate.far()
    gate.near()
    add_up_side(a_acc, wgf, xr, far_block, 2)
    up.far()
    up.near()
    add_up_side(b_acc, wuf, xr, far_block, 2)

    step_rows = 16

    def hidden_step(i):
        r = part_of(i, step_rows)
        a = a_acc[r]
        ha[part_of(dp * (rows // step_rows) + i, step_rows)] = (a * jax.nn.sigmoid(a) * b_acc[r]).astype(bf16)

    loop(rows // step_rows, hidden_step)
    hid = DpGather(links, ha.at[part_of(dp, rows)], row_slot(ha, rows))

    def y_block(block, n):
        def body(i):
            t = part_of(block(i // n_d) * n_d + i % n_d, d_tile)
            y_part[:, :, :, t] = dot(ha[part_of(dp, rows)], wdf[:, t], NN).reshape(RING, RING, tok, d_tile)
        loop(n * n_d, body)

    y_block(near_block, 6)
    down.far()
    down.near()
    add_down_side(far_block, 2)

    def grad_step(i):
        r = part_of(i, step_rows)
        own = part_of(dp * (rows // step_rows) + i, step_rows)
        a, b, g = a_acc[r], b_acc[r], g_acc[r]
        s = jax.nn.sigmoid(a)
        daa[own] = (g * b * (s * (1.0 + a * (1.0 - s)))).astype(bf16)
        dba[own] = (g * (a * s)).astype(bf16)

    loop(rows // step_rows, grad_step)
    dgate = DpGather(links, daa.at[part_of(dp, rows)], row_slot(daa, rows))
    dup = DpGather(links, dba.at[part_of(dp, rows)], row_slot(dba, rows))

    y_block(far_block, 2)
    n_buf = len(scat_bufs) // 4
    half = d // 2
    bufs = [scat_bufs[k * n_buf:(k + 1) * n_buf] for k in range(4)]
    ys = [Scatter(links, y_part, (0, half), True, bufs[0]), Scatter(links, y_part, (half, half), False, bufs[1])]
    gs = [Scatter(links, gx_part, (0, half), True, bufs[2]), Scatter(links, gx_part, (half, half), False, bufs[3])]
    for s in ys:
        s.start(0)

    def gx_step(i):
        t = part_of(i, d_tile)
        own = part_of(dp, rows)
        gx_part[:, :, :, t] = (dot(daa[own], wgf[t], NT) + dot(dba[own], wuf[t], NT)).reshape(RING, RING, tok, d_tile)

    n_half = half // d_tile
    loop(n_half, gx_step)
    for s in ys:
        s.forward(0)
    gs[0].start(0)
    loop(n_half, lambda i: gx_step(i + n_half))
    gs[1].start(0)

    links.sent_all()
    for j in range(N_DP):
        links.put(xc_ref.at[j], xr.at[:, :, :, pl.ds(j * d_loc, d_loc)])
        links.put(gc_ref.at[j], gr.at[:, :, :, pl.ds(j * d_loc, d_loc)])
    clear(acc_g, acc_u, acc_d)

    def add_wd(block, n):
        def body(i):
            j, t = block(i // n_ff), part_of(i % n_ff, ff_tile)
            acc_d[t] += dot(ha[part_of(j, rows), t], cols_of(gr, j), TN)
        loop(n * n_ff, body)

    def add_wup(acc, src, block, n):
        def body(i):
            j, t = block(i // n_ff), part_of(i % n_ff, ff_tile)
            acc[pl.ds(0, d_loc), t] += dot(cols_of(xr, j), src[part_of(j, rows), t], TN)
        loop(n * n_ff, body)

    hid.forward()
    for s in gs:
        s.forward(0)
    for s in ys:
        s.end(0)
        s.start(1)
    dgate.forward()
    for s in ys:
        s.forward(1)
    links.put_all()
    hid.near()
    add_wd(near_block, 6)

    def finish_rows(units, resid, out):
        for s, lo in zip(units, (0, half)):
            s.end(1)
            for h in (0, 1):
                step = min(CHUNK, s.half)
                for c in range(0, s.half, step):
                    cols = slice(lo + h * s.half + c, lo + h * s.half + c + step)
                    total = resid[:, cols].astype(jnp.float32) + s.result(h)[:, c:c + step]
                    out[:, cols] = total.astype(out.dtype)

    finish_rows(ys, x_ref, y_ref)
    dup.forward()
    for s in gs:
        s.end(0)
        s.start(1)
    dgate.near()
    add_wup(acc_g, daa, near_block, 6)
    hid.far()
    for s in gs:
        s.forward(1)
    hid.near()
    add_wd(far_block, 2)
    links.put(acc_d, gwd_ref)
    dup.near()
    add_wup(acc_u, dba, near_block, 6)
    dgate.far()
    finish_rows(gs, gy_ref, gx_ref)
    dgate.near()
    add_wup(acc_g, daa, far_block, 2)
    links.put(acc_g.at[pl.ds(0, d_loc)], gwg_ref)
    dup.far()
    dup.near()
    add_wup(acc_u, dba, far_block, 2)
    links.put(acc_u.at[pl.ds(0, d_loc)], gwu_ref)
    links.sent_all()
    links.put_all()


def solution(mesh):
    vmem = pl.BlockSpec(memory_space=VMEM)
    hbm = pl.BlockSpec(memory_space=pl.ANY)

    def local_step(x_loc, wg_loc, wu_loc, wd_loc, gy_loc):
        tok, d = x_loc.shape
        d_loc, ff = wg_loc.shape
        bf16, f32 = x_loc.dtype, jnp.float32
        sds = jax.ShapeDtypeStruct
        n_sem = 160
        rows = RING * RING * tok
        spread = sds((N_DP, RING, RING, tok, d_loc), bf16)
        up_rows = max(d_loc, 2 * rows)
        whole = pltpu.VMEM((N_DP * rows, ff), bf16)
        half1, half2 = (2, tok, d // 2), (tok, d // 4)
        scat = []
        for half in (half1, half2):
            scat += [pltpu.VMEM(half, f32)] * 2 + [pltpu.VMEM((2,) + half, f32)] * 2
        y_rows, gx_rows, grad_wg, grad_wu, grad_wd, _, _ = pl.pallas_call(
            mlp_kernel,
            out_shape=[sds((tok, d), bf16), sds((tok, d), bf16), sds((d_loc, ff), f32), sds((d_loc, ff), f32),
                       sds((ff, d_loc), f32), spread, spread],
            in_specs=[vmem] * 2 + [hbm] * 3,
            out_specs=[vmem] * 2 + [hbm] * 5,
            scratch_shapes=[pltpu.VMEM((d, ff), bf16)] * 2 + [pltpu.VMEM((ff, d), bf16)]
            + [pltpu.VMEM((RING, RING, tok, d), bf16)] * 2 + [whole] * 3
            + [pltpu.VMEM((up_rows, ff), f32)] * 2 + [pltpu.VMEM((ff, d_loc), f32)]
            + [pltpu.VMEM((RING, RING, tok, d), f32)] * 2 + scat * 4
            + [pltpu.SemaphoreType.DMA((n_sem,)), pltpu.SemaphoreType.DMA((n_sem,)), pltpu.SemaphoreType.DMA((32,))],
            compiler_params=pltpu.CompilerParams(collective_id=0, has_side_effects=True, vmem_limit_bytes=67043328),
            name="mlp",
        )(x_loc, gy_loc, wg_loc, wu_loc, wd_loc)
        return y_rows, gx_rows, grad_wg, grad_wu, grad_wd

    row_spec = P(("dp", "tp"), None)
    up_spec = P("dp", "tp")
    down_spec = P("tp", "dp")
    return jax.shard_map(local_step, mesh=mesh,
                         in_specs=(row_spec, up_spec, up_spec, down_spec, row_spec),
                         out_specs=(row_spec, row_spec, up_spec, up_spec, down_spec),
                         check_vma=False)
```

```python
import itertools

import jax
import jax.numpy as jnp
from jax import lax
from jax.experimental import pallas as pl
from jax.experimental.pallas import tpu as pltpu
from jax.sharding import PartitionSpec as P

RING = 4
N_DP = 2 * RING
VMEM = pltpu.MemorySpace.VMEM


class Links:
    def __init__(self, send_sem, recv_sem, local_sem):
        self.send_sem, self.recv_sem, self.local_sem = send_sem, recv_sem, local_sem
        self.n_remote = self.n_local = 0
        self.sent, self.local = [], []
        dp, tp = lax.axis_index("dp"), lax.axis_index("tp")
        self.dp, self.tp = dp, tp
        self.x, self.core = dp // 2, dp % 2
        self.z, self.y = tp // RING, tp % RING
        odd = self.x % 2
        self.xa = self.x + 1 - 2 * odd
        self.xb = (self.x + 3 + 2 * odd) % RING

    def at(self, pos, off):
        return (pos + off) % RING

    def device(self, axis, off):
        if axis == "x":
            return {"dp": 2 * self.at(self.x, off) + self.core, "tp": self.tp}
        if axis == "a":
            return {"dp": 2 * self.xa + self.core, "tp": self.tp}
        if axis == "b":
            return {"dp": 2 * self.xb + self.core, "tp": self.tp}
        if axis == "block":
            return {"dp": off, "tp": self.tp}
        if axis == "core":
            return {"dp": 2 * self.x + (1 - self.core), "tp": self.tp}
        if axis == "dp":
            return {"dp": (self.dp + off) % N_DP, "tp": self.tp}
        if axis == "z":
            return {"dp": self.dp, "tp": RING * self.at(self.z, off) + self.y}
        return {"dp": self.dp, "tp": RING * self.z + self.at(self.y, off)}

    def barrier(self, peers):
        sem = pltpu.get_barrier_semaphore()
        for axis, off in peers:
            pl.semaphore_signal(sem, inc=1, device_id=self.device(axis, off),
                                device_id_type=pl.DeviceIdType.MESH)
        pl.semaphore_wait(sem, len(peers))

    def send(self, src, dst, axis, off=0):
        k = self.n_remote
        self.n_remote += 1
        copy = pltpu.make_async_remote_copy(
            src_ref=src, dst_ref=dst, send_sem=self.send_sem.at[k], recv_sem=self.recv_sem.at[k],
            device_id=self.device(axis, off), device_id_type=pl.DeviceIdType.MESH)
        copy.start()
        self.sent.append(copy)
        return copy

    def put(self, src, dst):
        k = self.n_local
        self.n_local += 1
        copy = pltpu.make_async_copy(src, dst, self.local_sem.at[k])
        copy.start()
        self.local.append(copy)
        return copy

    def sent_all(self):
        for copy in self.sent:
            copy.wait_send()
        self.sent = []

    def put_all(self):
        for copy in self.local:
            copy.wait()
        self.local = []


def gather_start(links, own, block, axis, pos):
    right = links.send(own, block(pos, None), axis, 1)
    left = links.send(own, block(pos, None), axis, -1)
    return right, left


def gather_forward(links, copies, block, axis, pos):
    copies[0].wait_recv()
    from_left = links.at(pos, -1)
    right = links.send(block(from_left, 0), block(from_left, 0), axis, 1)
    copies[1].wait_recv()
    from_right = links.at(pos, 1)
    left = links.send(block(from_right, 1), block(from_right, 1), axis, -1)
    return right, left


def gather_end(copies):
    for copy in copies:
        copy.wait_recv()


class DpGather:
    def __init__(self, links, own, slot):
        self.links, self.slot = links, slot
        x, c = links.x, links.core
        self.block = lambda p, h: slot(2 * p + c, h)
        self.ring = gather_start(links, own, self.block, "x", x)
        self.mate = [links.send(own, slot(links.dp, None), "core")]

    def forward(self):
        links = self.links
        self.ring = gather_forward(links, self.ring, self.block, "x", links.x)
        for off in (-1, 1):
            b = self.block(links.at(links.x, off), None)
            self.mate.append(links.send(b, b, "core"))

    def near(self):
        gather_end(self.mate)
        self.mate = []

    def far(self):
        links = self.links
        far = links.at(links.x, 2)
        for h in (0, 1):
            self.ring[h].wait_recv()
            b = self.block(far, h)
            self.mate.append(links.send(b, b, "core"))


class PairGather:
    def __init__(self, links, own, slots):
        self.links, self.slots = links, slots
        c = links.core
        self.pair = [links.send(own(h), slots[h](2 + c), "ab"[h]) for h in (0, 1)]
        self.mate = [links.send(own(h), slots[h](c), "core") for h in (0, 1)]
        for h in (0, 1):
            links.put(own(h), slots[h](c))

    def forward(self):
        links = self.links
        for h in (0, 1):
            self.pair[h].wait_recv()
            s = self.slots[h](2 + links.core)
            self.mate.append(links.send(s, s, "core"))

    def near(self):
        gather_end(self.mate)


class Scatter:
    def __init__(self, links, part, slots, z_first, bufs):
        self.links, z, y = links, links.z, links.y
        half = part.shape[-1] // 2
        self.slots = slots
        n = pl.ds(slots[0], len(slots))
        if z_first:
            self.axes, self.pos = ("z", "y"), (z, y)
            first = lambda p, h: part.at[n, p, pl.ds(2 * h, 2)]
            second = lambda p, h: part.at[n, z, p, :, pl.ds(h * half, half)]
        else:
            self.axes, self.pos = ("y", "z"), (y, z)
            first = lambda p, h: part.at[n, pl.ds(2 * h, 2), p]
            second = lambda p, h: part.at[n, p, y, :, pl.ds(h * half, half)]
        self.block = (first, second)
        self.bufs = (bufs[:4], bufs[4:])

    def start(self, phase):
        links, block, axis, pos = self.links, self.block[phase], self.axes[phase], self.pos[phase]
        near0, near1, l_ref, r_ref = self.bufs[phase]
        far = links.at(pos, 2)
        self.first = (links.send(block(far, 0), near0, axis, 1), links.send(block(far, 1), near1, axis, -1))
        self.last = [links.send(block(links.at(pos, 1), 1), l_ref.at[1], axis, 1),
                     links.send(block(links.at(pos, -1), 0), r_ref.at[0], axis, -1)]

    def forward(self, phase):
        links, block, axis, pos = self.links, self.block[phase], self.axes[phase], self.pos[phase]
        near0, near1, l_ref, r_ref = self.bufs[phase]
        for copy, off, h, near, dst in ((self.first[0], 1, 0, near0, l_ref), (self.first[1], -1, 1, near1, r_ref)):
            copy.wait_recv()
            b = block(links.at(pos, off), h)
            add_into(b, [near])
            self.last.append(links.send(b, dst.at[h], axis, off))

    def end(self, phase):
        block, pos = self.block[phase], self.pos[phase]
        _, _, l_ref, r_ref = self.bufs[phase]
        gather_end(self.last)
        for h in (0, 1):
            add_into(block(pos, h), [l_ref.at[h], r_ref.at[h]])


TILE = 256


def add_into(dst, terms):
    for lead in itertools.product(*(range(n) for n in dst.shape[:-2])):
        total = dst[lead]
        for t in terms:
            total = total + t[lead]
        dst[lead] = total


def loop(n, body):
    def step(i, carry):
        body(i)
        return carry
    lax.fori_loop(0, n, step, 0)


def part_of(i, size):
    return pl.ds(pl.multiple_of(i * size, size), size)


NN = (((1,), (0,)), ((), ()))
NT = (((1,), (1,)), ((), ()))
TN = (((0,), (0,)), ((), ()))


def dot(a, b, dims):
    return lax.dot_general(a, b, dims, preferred_element_type=jnp.float32)


OWN, OWN_A, OWN_B, TOK_B, TOK_A, SECTIONS = 0, 2, 4, 6, 10, 14


def mlp_kernel(x_ref, gy_ref, wg_ref, wu_ref, wd_ref,
               y_ref, gx_ref, gwg_ref, gwu_ref, gwd_ref, xc_ref, gc_ref,
               wga, wgb, wua, wub, wda, wdb, xr, gr, xm, gm, q_out, q_in, ha, daa, dba,
               acc_g, acc_u, acc_d, y_part, gx_part, y_stage, gx_stage, *rest):
    scat_bufs, (send_sem, recv_sem, local_sem) = rest[:-3], rest[-3:]
    links = Links(send_sem, recv_sem, local_sem)
    dp, z, y, x, core = links.dp, links.z, links.y, links.x, links.core
    tok, d = x_ref.shape
    d_loc, ff = wg_ref.shape
    ffh = ff // 2
    rows = RING * RING * tok
    bf16 = x_ref.dtype
    links.barrier([("dp", o) for o in range(1, N_DP)] + [("z", 1), ("z", -1), ("y", 1), ("y", -1)])

    def d_of(ref, j, n=1):
        return ref.at[:, part_of(j, n * d_loc)]

    def section(ref, s, n):
        return ref.at[z, y, :, pl.ds(s * d_loc, n * d_loc)]

    def spread(src, dst):
        return [links.send(d_of(src, (dp + o) % N_DP), dst.at[dp], "dp", o) for o in range(1, N_DP)]

    opp = links.at(x, 2)

    def lend(src, dst):
        return [links.send(d_of(src, links.xb, 2), section(dst, TOK_B, 2), "b"),
                links.send(d_of(src, opp, 2), section(dst, TOK_B + 2, 2), "b"),
                links.send(d_of(src, links.xa, 2), section(dst, TOK_A, 2), "a"),
                links.send(d_of(src, opp, 2), section(dst, TOK_A + 2, 2), "a")]

    lent = [lend(x_ref, xr), lend(gy_ref, gr)]
    spreads = [spread(x_ref, xm), spread(gy_ref, gm)]
    gate = PairGather(links, lambda h: wg_ref.at[:, pl.ds(h * ffh, ffh)],
                      [lambda k: wga.at[part_of(k, d_loc)], lambda k: wgb.at[part_of(k, d_loc)]])
    up = PairGather(links, lambda h: wu_ref.at[:, pl.ds(h * ffh, ffh)],
                    [lambda k: wua.at[part_of(k, d_loc)], lambda k: wub.at[part_of(k, d_loc)]])
    down = PairGather(links, lambda h: wd_ref.at[pl.ds(h * ffh, ffh)],
                      [lambda k: wda.at[:, part_of(k, d_loc)], lambda k: wdb.at[:, part_of(k, d_loc)]])
    for src, dst, mine in ((x_ref, xr, xm), (gy_ref, gr, gm)):
        for s, j in ((OWN, x), (OWN_A, links.xa), (OWN_B, links.xb)):
            dst[z, y, :, s * d_loc:(s + 2) * d_loc] = src[:, part_of(j, 2 * d_loc)]
        mine[dp] = src[:, part_of(dp, d_loc)]

    row_half = SECTIONS * d_loc // 2

    def half_of(h):
        return pl.ds(h * row_half, row_half)

    def dp_half(h):
        return pl.ds(h * (N_DP // 2), N_DP // 2)

    def xr_first(p, h):
        return xr.at[p, y] if h is None else xr.at[p, y, :, half_of(h)]

    def xr_second(p, h):
        return xr.at[:, p] if h is None else xr.at[pl.ds(2 * h, 2), p]

    def gr_first(p, h):
        return gr.at[z, p] if h is None else gr.at[z, p, :, half_of(h)]

    def gr_second(p, h):
        return gr.at[p] if h is None else gr.at[p, pl.ds(2 * h, 2)]

    def xc_first(p, h):
        return xc_ref.at[:, p, y] if h is None else xc_ref.at[dp_half(h), p, y]

    def xc_second(p, h):
        return xc_ref.at[:, :, p] if h is None else xc_ref.at[dp_half(h), :, p]

    def gc_first(p, h):
        return gc_ref.at[:, z, p] if h is None else gc_ref.at[dp_half(h), z, p]

    def gc_second(p, h):
        return gc_ref.at[:, p] if h is None else gc_ref.at[dp_half(h), p]

    row_sends = []

    def start(own, block, axis, pos):
        copies = gather_start(links, own, block, axis, pos)
        row_sends.extend(copies)
        return copies

    def forward(copies, block, axis, pos):
        copies = gather_forward(links, copies, block, axis, pos)
        row_sends.extend(copies)
        return copies

    gather_end(lent[0])
    rx = start(xr_first(z, None), xr_first, "z", z)
    gather_end(lent[1])
    rg = start(gr_first(y, None), gr_first, "y", y)
    for copies in spreads:
        gather_end(copies)
    links.put_all()
    own_cols = [links.put(xm, xc_first(z, None)), links.put(gm, gc_first(y, None))]
    rx = forward(rx, xr_first, "z", z)
    rg = forward(rg, gr_first, "y", y)
    gather_end(rx)
    rx = start(xr_second(y, None), xr_second, "y", y)
    gather_end(rg)
    rg = start(gr_second(z, None), gr_second, "z", z)
    gate.forward()
    rx = forward(rx, xr_second, "y", y)
    rg = forward(rg, gr_second, "z", z)
    links.put_all()
    cx = gather_start(links, xm, xc_first, "z", z)
    cg = gather_start(links, gm, gc_first, "y", y)
    up.forward()
    gather_end(rx)

    accs = (acc_g.at[pl.ds(0, rows)], acc_g.at[pl.ds(rows, rows)], acc_u.at[pl.ds(0, rows)])
    tile = min(TILE, ffh)
    n_tile = ffh // tile

    def take(ref, s, n):
        return ref[:, :, :, s * d_loc:(s + n) * d_loc].reshape(rows, n * d_loc)

    def product(src, s, n, w, first, t, down_side):
        if down_side:
            return dot(take(src, s, n), w[t, first * d_loc:(first + n) * d_loc], NT)
        return dot(take(src, s, n), w[first * d_loc:(first + n) * d_loc, t], NN)

    def lend_sums(k, src, wa, wb, down_side):
        def body(i):
            t = part_of(i, tile)
            q_out[k, 0, :, t] = product(src, TOK_B, 4, wa, 0, t, down_side)
            q_out[k, 1, :, t] = product(src, TOK_A, 4, wb, 0, t, down_side)
        loop(n_tile, body)
        return [links.send(q_out.at[k, 0], q_in.at[k, 0], "b"), links.send(q_out.at[k, 1], q_in.at[k, 1], "a")]

    def own_sums(k, src, wa, wb, down_side):
        def body(i):
            t = part_of(i, tile)
            accs[k][:, t] = product(src, OWN, 4, wa, 0, t, down_side)
            accs[k][:, part_of(i + n_tile, tile)] = (product(src, OWN, 2, wb, 0, t, down_side)
                                                     + product(src, OWN_B, 2, wb, 2, t, down_side))
        loop(n_tile, body)

    gate.near()
    qa = lend_sums(0, xr, wga, wgb, False)
    up.near()
    qb = lend_sums(1, xr, wua, wub, False)
    gather_end(rg)
    down.forward()
    down.near()
    qg = lend_sums(2, gr, wda, wdb, True)
    cx = gather_forward(links, cx, xc_first, "z", z)
    cg = gather_forward(links, cg, gc_first, "y", y)
    own_sums(0, xr, wga, wgb, False)
    own_sums(1, xr, wua, wub, False)
    gather_end(cx)
    cx = gather_start(links, xc_second(y, None), xc_second, "y", y)
    gather_end(cg)
    cg = gather_start(links, gc_second(z, None), gc_second, "z", z)
    own_sums(2, gr, wda, wdb, True)

    step_rows = 16

    def gate_loop(body):
        def step(i):
            r = part_of(i, step_rows)
            own = part_of(dp * (rows // step_rows) + i, step_rows)
            for h in (0, 1):
                cols = pl.ds(h * ffh, ffh)
                body(own, cols, lambda k: accs[k][r, cols] + q_in[k, h, r])
        loop(rows // step_rows, step)

    def hidden_body(own, cols, value):
        a = value(0)
        ha[own, cols] = (a * jax.nn.sigmoid(a) * value(1)).astype(bf16)

    gather_end(qa)
    gather_end(qb)
    gate_loop(hidden_body)
    mine = part_of(dp, rows)

    def row_slot(ref):
        def slot(j, h):
            if h is None:
                return ref.at[part_of(j, rows)]
            return ref.at[part_of(2 * j + h, rows // 2)]
        return slot

    hid = DpGather(links, ha.at[mine], row_slot(ha))
    cx = gather_forward(links, cx, xc_second, "y", y)
    cg = gather_forward(links, cg, gc_second, "z", z)

    def grad_body(own, cols, value):
        a, g = value(0), value(2)
        s = jax.nn.sigmoid(a)
        daa[own, cols] = (g * value(1) * (s * (1.0 + a * (1.0 - s)))).astype(bf16)
        dba[own, cols] = (g * (a * s)).astype(bf16)

    gather_end(qg)
    gate_loop(grad_body)
    dgate = DpGather(links, daa.at[mine], row_slot(daa))
    dup = DpGather(links, dba.at[mine], row_slot(dba))

    gather_end(cx)
    gather_end(cg)
    for copy in row_sends:
        copy.wait_send()
    links.sent = [c for c in links.sent if not any(c is r for r in row_sends)]
    for j in range(N_DP):
        links.put(xc_ref.at[j], xr.at[:, :, :, pl.ds(j * d_loc, d_loc)])
        links.put(gc_ref.at[j], gr.at[:, :, :, pl.ds(j * d_loc, d_loc)])

    def clear(*refs):
        for ref in refs:
            n, step = ref.shape[0], min(16, ref.shape[0])

            def body(i):
                ref[part_of(i, step)] = jnp.zeros((step, ref.shape[1]), jnp.float32)
            loop(n // step, body)

    clear(acc_g, acc_u, acc_d)

    def block_of(s):
        far = s // 6
        q = s % 3
        chip = (1 - far) * (q + q // 2) + far * 2
        other = (1 - far) * ((s // 3) % 2) + far * (s % 2)
        return 2 * ((x + chip) % RING) + (core + other) % 2

    d_tile = min(TILE, d_loc)
    n_d = d_loc // d_tile
    ff_tile = min(TILE, ff)
    n_ff = ff // ff_tile
    low, high = pl.ds(0, ffh), pl.ds(ffh, ffh)
    torus = (RING, RING, tok)

    def y_blocks(lo, n):
        def body(i):
            s = lo + i // n_d
            r, t = part_of(block_of(s), rows), part_of(i % n_d, d_tile)
            w = part_of(core * n_d + i % n_d, d_tile)
            y_part[s, :, :, :, t] = (dot(ha[r, low], wda[:, w], NN) + dot(ha[r, high], wdb[:, w], NN)).reshape(
                torus + (d_tile,))
        loop(n * n_d, body)

    def gx_blocks(lo, n):
        def body(i):
            s = lo + i // n_d
            r, t = part_of(block_of(s), rows), part_of(i % n_d, d_tile)
            w = part_of(core * n_d + i % n_d, d_tile)
            gx_part[s, :, :, :, t] = (dot(daa[r, low], wga[w], NT) + dot(daa[r, high], wgb[w], NT)
                                      + dot(dba[r, low], wua[w], NT) + dot(dba[r, high], wub[w], NT)).reshape(
                torus + (d_tile,))
        loop(n * n_d, body)

    def cols_of(ref, j):
        return ref[:, :, :, part_of(j, d_loc)].reshape(rows, d_loc)

    def add_wd(lo, n):
        def body(i):
            j, t = block_of(lo + i // n_ff), part_of(i % n_ff, ff_tile)
            acc_d[t] += dot(ha[part_of(j, rows), t], cols_of(gr, j), TN)
        loop(n * n_ff, body)

    def add_wup(acc, src, lo, n):
        def body(i):
            j, t = block_of(lo + i // n_ff), part_of(i % n_ff, ff_tile)
            acc[pl.ds(0, d_loc), t] += dot(cols_of(xr, j), src[part_of(j, rows), t], TN)
        loop(n * n_ff, body)

    n_buf = 8

    def units(part, k):
        bufs = [scat_bufs[(4 * k + u) * n_buf:(4 * k + u + 1) * n_buf] for u in range(4)]
        near = [Scatter(links, part, (0, 1, 2), True, bufs[0]), Scatter(links, part, (3, 4, 5), False, bufs[1])]
        return near, [Scatter(links, part, (6,), True, bufs[2]), Scatter(links, part, (7,), False, bufs[3])]

    y_near, y_far = units(y_part, 0)
    g_near, g_far = units(gx_part, 1)
    returns = []

    def finish(group, part, resid, stage, out):
        for unit in group:
            unit.end(1)
            for s in unit.slots:
                j = block_of(s)
                piece = (resid[j].astype(jnp.float32) + part[s, z, y]).astype(bf16)
                if s == 0:
                    out[:, part_of(dp, d_loc)] = piece
                else:
                    stage[s] = piece
        for unit in group:
            for s in unit.slots:
                if s:
                    returns.append(links.send(stage.at[s], out.at[:, part_of(dp, d_loc)], "block", block_of(s)))

    def each(group, *steps):
        for name, phase in steps:
            for unit in group:
                getattr(unit, name)(phase)

    hid.forward()
    hid.near()
    y_blocks(0, 6)
    each(y_near, ("start", 0))
    links.put_all()
    add_wd(0, 6)
    each(y_near, ("forward", 0))
    dgate.forward()
    each(y_near, ("end", 0), ("start", 1))
    dup.forward()
    dgate.near()
    dup.near()
    gx_blocks(0, 6)
    each(g_near, ("start", 0))
    each(y_near, ("forward", 1))
    hid.far()
    hid.near()
    y_blocks(6, 2)
    each(y_far, ("start", 0))
    add_wup(acc_g, daa, 0, 6)
    each(g_near, ("forward", 0))
    finish(y_near, y_part, xm, y_stage, y_ref)
    dgate.far()
    each(y_far, ("forward", 0))
    add_wup(acc_u, dba, 0, 6)
    dup.far()
    dgate.near()
    dup.near()
    gx_blocks(6, 2)
    each(g_far, ("start", 0))
    each(y_far, ("end", 0), ("start", 1))
    add_wd(6, 2)
    links.put(acc_d, gwd_ref)
    each(g_near, ("end", 0), ("start", 1))
    each(g_far, ("forward", 0))
    each(y_far, ("forward", 1))
    add_wup(acc_g, daa, 6, 2)
    links.put(acc_g.at[pl.ds(0, d_loc)], gwg_ref)
    each(g_far, ("end", 0), ("start", 1))
    each(g_near, ("forward", 1))
    each(g_far, ("forward", 1))
    finish(y_far, y_part, xm, y_stage, y_ref)
    finish(g_near, gx_part, gm, gx_stage, gx_ref)
    finish(g_far, gx_part, gm, gx_stage, gx_ref)
    add_wup(acc_u, dba, 6, 2)
    links.put(acc_u.at[pl.ds(0, d_loc)], gwu_ref)
    gather_end(returns)
    links.sent_all()
    links.put_all()


PIECES = 4


def copy_kernel(*refs):
    n = (len(refs) - 2) // 3
    ins, outs, bufs, (in_sem, out_sem) = refs[:n], refs[n:2 * n], refs[2 * n:3 * n], refs[3 * n:]
    loads, stores = [], []
    for k in range(n):
        pieces = PIECES if ins[k].shape[0] >= 128 else 1
        size = ins[k].shape[0] // pieces
        for p in range(pieces):
            part, sem = pl.ds(p * size, size), k * PIECES + p
            loads.append(pltpu.make_async_copy(ins[k].at[part], bufs[k].at[part], in_sem.at[sem]))
            stores.append(pltpu.make_async_copy(bufs[k].at[part], outs[k].at[part], out_sem.at[sem]))
    for load in loads:
        load.start()
    for load, store in zip(loads, stores):
        load.wait()
        store.start()
    for store in stores:
        store.wait()


def solution(mesh):
    vmem = pl.BlockSpec(memory_space=VMEM)
    hbm = pl.BlockSpec(memory_space=pl.ANY)

    def local_step(x_loc, wg_loc, wu_loc, wd_loc, gy_loc):
        tok, d = x_loc.shape
        d_loc, ff = wg_loc.shape
        ffh = ff // 2
        bf16, f32 = x_loc.dtype, jnp.float32
        sds = jax.ShapeDtypeStruct
        n_sem = 224
        rows = RING * RING * tok
        spread = sds((N_DP, RING, RING, tok, d_loc), bf16)
        up_rows = max(d_loc, 2 * rows)
        whole = pltpu.VMEM((N_DP * rows, ff), bf16)
        mine = pltpu.VMEM((N_DP, tok, d_loc), bf16)
        scat = []
        for n in (3, 3, 1, 1):
            for half in ((n, 2, tok, d_loc), (n, tok, d_loc // 2)):
                scat += [pltpu.VMEM(half, f32)] * 2 + [pltpu.VMEM((2,) + half, f32)] * 2
        results = [sds((tok, d), bf16), sds((tok, d), bf16), sds((d_loc, ff), f32), sds((d_loc, ff), f32),
                   sds((ff, d_loc), f32)]
        outs = pl.pallas_call(
            mlp_kernel,
            out_shape=results + [spread, spread],
            in_specs=[vmem] * 2 + [hbm] * 3,
            out_specs=[vmem] * 2 + [hbm] * 5,
            scratch_shapes=[pltpu.VMEM((4 * d_loc, ffh), bf16)] * 4 + [pltpu.VMEM((ffh, 4 * d_loc), bf16)] * 2
            + [pltpu.VMEM((RING, RING, tok, SECTIONS * d_loc), bf16)] * 2 + [mine] * 2
            + [pltpu.VMEM((3, 2, rows, ffh), f32)] * 2 + [whole] * 3
            + [pltpu.VMEM((up_rows, ff), f32)] * 2 + [pltpu.VMEM((ff, d_loc), f32)]
            + [pltpu.VMEM((N_DP, RING, RING, tok, d_loc), f32)] * 2 + [mine] * 2 + scat * 2
            + [pltpu.SemaphoreType.DMA((n_sem,)), pltpu.SemaphoreType.DMA((n_sem,)), pltpu.SemaphoreType.DMA((32,))],
            compiler_params=pltpu.CompilerParams(collective_id=0, has_side_effects=True, vmem_limit_bytes=67043328),
            name="mlp",
        )(x_loc, gy_loc, wg_loc, wu_loc, wd_loc)[:5]
        return pl.pallas_call(
            copy_kernel,
            out_shape=results,
            in_specs=[hbm] * 5,
            out_specs=[hbm] * 5,
            scratch_shapes=[pltpu.VMEM(r.shape, r.dtype) for r in results]
            + [pltpu.SemaphoreType.DMA((5 * PIECES,))] * 2,
            name="results",
        )(*outs)

    row_spec = P(("dp", "tp"), None)
    up_spec = P("dp", "tp")
    down_spec = P("tp", "dp")
    return jax.shard_map(local_step, mesh=mesh,
                         in_specs=(row_spec, up_spec, up_spec, down_spec, row_spec),
                         out_specs=(row_spec, row_spec, up_spec, up_spec, down_spec),
                         check_vma=False)
```

```python
import itertools

import jax
import jax.numpy as jnp
from jax import lax
from jax.experimental import pallas as pl
from jax.experimental.pallas import tpu as pltpu
from jax.sharding import PartitionSpec as P

RING = 4
N_DP = 2 * RING
VMEM = pltpu.MemorySpace.VMEM


class Links:
    def __init__(self, send_sem, recv_sem, local_sem):
        self.send_sem, self.recv_sem, self.local_sem = send_sem, recv_sem, local_sem
        self.n_remote = self.n_local = 0
        self.sent, self.local = [], []
        dp, tp = lax.axis_index("dp"), lax.axis_index("tp")
        self.dp, self.tp = dp, tp
        self.x, self.core = dp // 2, dp % 2
        self.z, self.y = tp // RING, tp % RING
        odd = self.x % 2
        self.xa = self.x + 1 - 2 * odd
        self.xb = (self.x + 3 + 2 * odd) % RING

    def at(self, pos, off):
        return (pos + off) % RING

    def device(self, axis, off):
        if axis == "x":
            return {"dp": 2 * self.at(self.x, off) + self.core, "tp": self.tp}
        if axis == "a":
            return {"dp": 2 * self.xa + self.core, "tp": self.tp}
        if axis == "b":
            return {"dp": 2 * self.xb + self.core, "tp": self.tp}
        if axis == "block":
            return {"dp": off, "tp": self.tp}
        if axis == "core":
            return {"dp": 2 * self.x + (1 - self.core), "tp": self.tp}
        if axis == "dp":
            return {"dp": (self.dp + off) % N_DP, "tp": self.tp}
        if axis == "z":
            return {"dp": self.dp, "tp": RING * self.at(self.z, off) + self.y}
        return {"dp": self.dp, "tp": RING * self.z + self.at(self.y, off)}

    def barrier(self, peers):
        sem = pltpu.get_barrier_semaphore()
        for axis, off in peers:
            pl.semaphore_signal(sem, inc=1, device_id=self.device(axis, off),
                                device_id_type=pl.DeviceIdType.MESH)
        pl.semaphore_wait(sem, len(peers))

    def send(self, src, dst, axis, off=0):
        k = self.n_remote
        self.n_remote += 1
        copy = pltpu.make_async_remote_copy(
            src_ref=src, dst_ref=dst, send_sem=self.send_sem.at[k], recv_sem=self.recv_sem.at[k],
            device_id=self.device(axis, off), device_id_type=pl.DeviceIdType.MESH)
        copy.start()
        self.sent.append(copy)
        return copy

    def put(self, src, dst):
        k = self.n_local
        self.n_local += 1
        copy = pltpu.make_async_copy(src, dst, self.local_sem.at[k])
        copy.start()
        self.local.append(copy)
        return copy

    def sent_all(self):
        for copy in self.sent:
            copy.wait_send()
        self.sent = []

    def put_all(self):
        for copy in self.local:
            copy.wait()
        self.local = []


def gather_start(links, own, block, axis, pos):
    right = links.send(own, block(pos, None), axis, 1)
    left = links.send(own, block(pos, None), axis, -1)
    return right, left


def gather_forward(links, copies, block, axis, pos):
    copies[0].wait_recv()
    from_left = links.at(pos, -1)
    right = links.send(block(from_left, 0), block(from_left, 0), axis, 1)
    copies[1].wait_recv()
    from_right = links.at(pos, 1)
    left = links.send(block(from_right, 1), block(from_right, 1), axis, -1)
    return right, left


def gather_end(copies):
    for copy in copies:
        copy.wait_recv()


class DpGather:
    def __init__(self, links, own, slot):
        self.links, self.slot = links, slot
        x, c = links.x, links.core
        self.block = lambda p, h: slot(2 * p + c, h)
        self.ring = gather_start(links, own, self.block, "x", x)
        self.mate = [links.send(own, slot(links.dp, None), "core")]

    def forward(self):
        links = self.links
        self.ring = gather_forward(links, self.ring, self.block, "x", links.x)
        for off in (-1, 1):
            b = self.block(links.at(links.x, off), None)
            self.mate.append(links.send(b, b, "core"))

    def near(self):
        gather_end(self.mate)
        self.mate = []

    def far(self):
        links = self.links
        far = links.at(links.x, 2)
        for h in (0, 1):
            self.ring[h].wait_recv()
            b = self.block(far, h)
            self.mate.append(links.send(b, b, "core"))


class PairGather:
    def __init__(self, links, own, slots):
        self.links, self.slots = links, slots
        c = links.core
        self.pair = [links.send(own(h), slots[h](2 + c), "ab"[h]) for h in (0, 1)]
        self.mate = [links.send(own(h), slots[h](c), "core") for h in (0, 1)]
        for h in (0, 1):
            links.put(own(h), slots[h](c))

    def forward(self):
        links = self.links
        for h in (0, 1):
            self.pair[h].wait_recv()
            s = self.slots[h](2 + links.core)
            self.mate.append(links.send(s, s, "core"))

    def near(self):
        gather_end(self.mate)


class Rows:
    def __init__(self, links, ref, lo, width, z_first):
        self.links, z, y = links, links.z, links.y
        half = width // 2
        cols = pl.ds(lo, width)
        if z_first:
            self.axes, self.pos = ("z", "y"), (z, y)
            first = lambda p, h: ref.at[p, y, :, cols if h is None else pl.ds(lo + h * half, half)]
            second = lambda p, h: ref.at[slice(None) if h is None else pl.ds(2 * h, 2), p, :, cols]
        else:
            self.axes, self.pos = ("y", "z"), (y, z)
            first = lambda p, h: ref.at[z, p, :, cols if h is None else pl.ds(lo + h * half, half)]
            second = lambda p, h: ref.at[p, slice(None) if h is None else pl.ds(2 * h, 2), :, cols]
        self.block = (first, second)
        self.sent = []

    def start(self, phase):
        block, pos = self.block[phase], self.pos[phase]
        self.copies = gather_start(self.links, block(pos, None), block, self.axes[phase], pos)
        self.sent.extend(self.copies)

    def forward(self, phase):
        self.copies = gather_forward(self.links, self.copies, self.block[phase], self.axes[phase], self.pos[phase])
        self.sent.extend(self.copies)

    def end(self, phase):
        gather_end(self.copies)


class Scatter:
    def __init__(self, links, part, slots, z_first, bufs):
        self.links, z, y = links, links.z, links.y
        half = part.shape[-1] // 2
        self.slots = slots
        n = pl.ds(slots[0], len(slots))
        if z_first:
            self.axes, self.pos = ("z", "y"), (z, y)
            first = lambda p, h: part.at[n, p, pl.ds(2 * h, 2)]
            second = lambda p, h: part.at[n, z, p, :, pl.ds(h * half, half)]
        else:
            self.axes, self.pos = ("y", "z"), (y, z)
            first = lambda p, h: part.at[n, pl.ds(2 * h, 2), p]
            second = lambda p, h: part.at[n, p, y, :, pl.ds(h * half, half)]
        self.block = (first, second)
        self.bufs = (bufs[:4], bufs[4:])

    def start(self, phase):
        links, block, axis, pos = self.links, self.block[phase], self.axes[phase], self.pos[phase]
        near0, near1, l_ref, r_ref = self.bufs[phase]
        far = links.at(pos, 2)
        self.first = (links.send(block(far, 0), near0, axis, 1), links.send(block(far, 1), near1, axis, -1))
        self.last = [links.send(block(links.at(pos, 1), 1), l_ref.at[1], axis, 1),
                     links.send(block(links.at(pos, -1), 0), r_ref.at[0], axis, -1)]

    def forward(self, phase):
        links, block, axis, pos = self.links, self.block[phase], self.axes[phase], self.pos[phase]
        near0, near1, l_ref, r_ref = self.bufs[phase]
        for copy, off, h, near, dst in ((self.first[0], 1, 0, near0, l_ref), (self.first[1], -1, 1, near1, r_ref)):
            copy.wait_recv()
            b = block(links.at(pos, off), h)
            add_into(b, [near])
            self.last.append(links.send(b, dst.at[h], axis, off))

    def end(self, phase):
        block, pos = self.block[phase], self.pos[phase]
        _, _, l_ref, r_ref = self.bufs[phase]
        gather_end(self.last)
        for h in (0, 1):
            add_into(block(pos, h), [l_ref.at[h], r_ref.at[h]])


TILE = 256


def add_into(dst, terms):
    for lead in itertools.product(*(range(n) for n in dst.shape[:-2])):
        total = dst[lead]
        for t in terms:
            total = total + t[lead]
        dst[lead] = total


def loop(n, body):
    def step(i, carry):
        body(i)
        return carry
    lax.fori_loop(0, n, step, 0)


def part_of(i, size):
    return pl.ds(pl.multiple_of(i * size, size), size)


NN = (((1,), (0,)), ((), ()))
NT = (((1,), (1,)), ((), ()))
TN = (((0,), (0,)), ((), ()))


def dot(a, b, dims):
    return lax.dot_general(a, b, dims, preferred_element_type=jnp.float32)


OWN, OWN_A, OWN_B, TOK_B, TOK_A, SECTIONS = 0, 2, 4, 6, 10, 14


def mlp_kernel(x_ref, gy_ref, wg_ref, wu_ref, wd_ref,
               y_ref, gx_ref, gwg_ref, gwu_ref, gwd_ref, xc_ref, gc_ref,
               wga, wgb, wua, wub, wda, wdb, xr, gr, xm, gm, q_out, q_in, ha, daa, dba,
               acc_g, acc_u, acc_d, y_part, gx_part, y_stage, gx_stage, *rest):
    scat_bufs, (send_sem, recv_sem, local_sem) = rest[:-3], rest[-3:]
    links = Links(send_sem, recv_sem, local_sem)
    dp, z, y, x, core = links.dp, links.z, links.y, links.x, links.core
    tok, d = x_ref.shape
    d_loc, ff = wg_ref.shape
    ffh = ff // 2
    rows = RING * RING * tok
    bf16 = x_ref.dtype
    links.barrier([("dp", o) for o in range(1, N_DP)] + [("z", 1), ("z", -1), ("y", 1), ("y", -1)])

    def d_of(ref, j, n=1):
        return ref.at[:, part_of(j, n * d_loc)]

    def section(ref, s, n):
        return ref.at[z, y, :, pl.ds(s * d_loc, n * d_loc)]

    def spread(src, dst):
        return [links.send(d_of(src, (dp + o) % N_DP), dst.at[dp], "dp", o) for o in range(1, N_DP)]

    opp = links.at(x, 2)

    def lend(src, dst):
        return [links.send(d_of(src, links.xb, 2), section(dst, TOK_B, 2), "b"),
                links.send(d_of(src, opp, 2), section(dst, TOK_B + 2, 2), "b"),
                links.send(d_of(src, links.xa, 2), section(dst, TOK_A, 2), "a"),
                links.send(d_of(src, opp, 2), section(dst, TOK_A + 2, 2), "a")]

    lent = [lend(x_ref, xr), lend(gy_ref, gr)]
    gate = PairGather(links, lambda h: wg_ref.at[:, pl.ds(h * ffh, ffh)],
                      [lambda k: wga.at[part_of(k, d_loc)], lambda k: wgb.at[part_of(k, d_loc)]])
    up = PairGather(links, lambda h: wu_ref.at[:, pl.ds(h * ffh, ffh)],
                    [lambda k: wua.at[part_of(k, d_loc)], lambda k: wub.at[part_of(k, d_loc)]])
    spreads = [spread(x_ref, xm), spread(gy_ref, gm)]
    down = PairGather(links, lambda h: wd_ref.at[pl.ds(h * ffh, ffh)],
                      [lambda k: wda.at[:, part_of(k, d_loc)], lambda k: wdb.at[:, part_of(k, d_loc)]])
    for src, dst, mine in ((x_ref, xr, xm), (gy_ref, gr, gm)):
        for s, j in ((OWN, x), (OWN_A, links.xa), (OWN_B, links.xb)):
            dst[z, y, :, s * d_loc:(s + 2) * d_loc] = src[:, part_of(j, 2 * d_loc)]
        mine[dp] = src[:, part_of(dp, d_loc)]

    def each(group, *steps):
        for name, phase in steps:
            for unit in group:
                getattr(unit, name)(phase)

    row_half = SECTIONS * d_loc // 2
    x_rows = [Rows(links, xr, 0, row_half, True), Rows(links, xr, row_half, row_half, False)]
    g_rows = [Rows(links, gr, 0, row_half, True), Rows(links, gr, row_half, row_half, False)]

    def dp_half(h):
        return pl.ds(h * (N_DP // 2), N_DP // 2)

    def xc_first(p, h):
        return xc_ref.at[:, p, y] if h is None else xc_ref.at[dp_half(h), p, y]

    def xc_second(p, h):
        return xc_ref.at[:, :, p] if h is None else xc_ref.at[dp_half(h), :, p]

    def gc_first(p, h):
        return gc_ref.at[:, z, p] if h is None else gc_ref.at[dp_half(h), z, p]

    def gc_second(p, h):
        return gc_ref.at[:, p] if h is None else gc_ref.at[dp_half(h), p]

    gather_end(lent[0])
    each(x_rows, ("start", 0))
    gather_end(lent[1])
    each(x_rows, ("forward", 0), ("end", 0), ("start", 1))
    each(g_rows, ("start", 0))
    each(x_rows, ("forward", 1))
    links.put_all()
    gate.forward()
    each(g_rows, ("forward", 0), ("end", 0), ("start", 1))
    each(x_rows, ("end", 1))

    accs = (acc_g.at[pl.ds(0, rows)], acc_g.at[pl.ds(rows, rows)], acc_u.at[pl.ds(0, rows)])
    tile = min(TILE, ffh)
    n_tile = ffh // tile

    def take(ref, s, n):
        return ref[:, :, :, s * d_loc:(s + n) * d_loc].reshape(rows, n * d_loc)

    def product(src, s, n, w, first, t, down_side):
        if down_side:
            return dot(take(src, s, n), w[t, first * d_loc:(first + n) * d_loc], NT)
        return dot(take(src, s, n), w[first * d_loc:(first + n) * d_loc, t], NN)

    def lend_sums(k, src, wa, wb, down_side):
        def body(i):
            t = part_of(i, tile)
            q_out[k, 0, :, t] = product(src, TOK_B, 4, wa, 0, t, down_side)
            q_out[k, 1, :, t] = product(src, TOK_A, 4, wb, 0, t, down_side)
        loop(n_tile, body)
        return [links.send(q_out.at[k, 0], q_in.at[k, 0], "b"), links.send(q_out.at[k, 1], q_in.at[k, 1], "a")]

    def own_sums(k, src, wa, wb, down_side):
        def body(i):
            t = part_of(i, tile)
            accs[k][:, t] = product(src, OWN, 4, wa, 0, t, down_side)
            accs[k][:, part_of(i + n_tile, tile)] = (product(src, OWN, 2, wb, 0, t, down_side)
                                                     + product(src, OWN_B, 2, wb, 2, t, down_side))
        loop(n_tile, body)

    gate.near()
    qa = lend_sums(0, xr, wga, wgb, False)
    up.forward()
    up.near()
    qb = lend_sums(1, xr, wua, wub, False)
    for copies in spreads:
        gather_end(copies)
    links.put(xm, xc_first(z, None))
    links.put(gm, gc_first(y, None))
    each(g_rows, ("forward", 1))
    cx = gather_start(links, xm, xc_first, "z", z)
    cg = gather_start(links, gm, gc_first, "y", y)
    own_sums(0, xr, wga, wgb, False)
    own_sums(1, xr, wua, wub, False)
    down.forward()
    each(g_rows, ("end", 1))
    down.near()
    qg = lend_sums(2, gr, wda, wdb, True)
    cx = gather_forward(links, cx, xc_first, "z", z)
    cg = gather_forward(links, cg, gc_first, "y", y)
    own_sums(2, gr, wda, wdb, True)
    links.put_all()

    step_rows = 16

    def gate_loop(body):
        def step(i):
            r = part_of(i, step_rows)
            own = part_of(dp * (rows // step_rows) + i, step_rows)
            for h in (0, 1):
                cols = pl.ds(h * ffh, ffh)
                body(own, cols, lambda k: accs[k][r, cols] + q_in[k, h, r])
        loop(rows // step_rows, step)

    def hidden_body(own, cols, value):
        a = value(0)
        ha[own, cols] = (a * jax.nn.sigmoid(a) * value(1)).astype(bf16)

    gather_end(qa)
    gather_end(qb)
    gate_loop(hidden_body)
    mine = part_of(dp, rows)

    def row_slot(ref):
        def slot(j, h):
            if h is None:
                return ref.at[part_of(j, rows)]
            return ref.at[part_of(2 * j + h, rows // 2)]
        return slot

    hid = DpGather(links, ha.at[mine], row_slot(ha))
    gather_end(cx)
    cx = gather_start(links, xc_second(y, None), xc_second, "y", y)
    gather_end(cg)
    cg = gather_start(links, gc_second(z, None), gc_second, "z", z)

    def grad_body(own, cols, value):
        a, g = value(0), value(2)
        s = jax.nn.sigmoid(a)
        daa[own, cols] = (g * value(1) * (s * (1.0 + a * (1.0 - s)))).astype(bf16)
        dba[own, cols] = (g * (a * s)).astype(bf16)

    gather_end(qg)
    gate_loop(grad_body)
    dgate = DpGather(links, daa.at[mine], row_slot(daa))
    dup = DpGather(links, dba.at[mine], row_slot(dba))

    cx = gather_forward(links, cx, xc_second, "y", y)
    cg = gather_forward(links, cg, gc_second, "z", z)

    def clear(*refs):
        for ref in refs:
            n, step = ref.shape[0], min(16, ref.shape[0])

            def body(i):
                ref[part_of(i, step)] = jnp.zeros((step, ref.shape[1]), jnp.float32)
            loop(n // step, body)

    clear(acc_g, acc_u, acc_d)

    def block_of(s):
        far = s // 6
        q = s % 3
        chip = (1 - far) * (q + q // 2) + far * 2
        other = (1 - far) * ((s // 3) % 2) + far * (s % 2)
        return 2 * ((x + chip) % RING) + (core + other) % 2

    d_tile = min(TILE, d_loc)
    n_d = d_loc // d_tile
    ff_tile = min(TILE, ff)
    n_ff = ff // ff_tile
    low, high = pl.ds(0, ffh), pl.ds(ffh, ffh)
    torus = (RING, RING, tok)

    def y_blocks(lo, n):
        def body(i):
            s = lo + i // n_d
            r, t = part_of(block_of(s), rows), part_of(i % n_d, d_tile)
            w = part_of(core * n_d + i % n_d, d_tile)
            y_part[s, :, :, :, t] = (dot(ha[r, low], wda[:, w], NN) + dot(ha[r, high], wdb[:, w], NN)).reshape(
                torus + (d_tile,))
        loop(n * n_d, body)

    def gx_blocks(lo, n):
        def body(i):
            s = lo + i // n_d
            r, t = part_of(block_of(s), rows), part_of(i % n_d, d_tile)
            w = part_of(core * n_d + i % n_d, d_tile)
            gx_part[s, :, :, :, t] = (dot(daa[r, low], wga[w], NT) + dot(daa[r, high], wgb[w], NT)
                                      + dot(dba[r, low], wua[w], NT) + dot(dba[r, high], wub[w], NT)).reshape(
                torus + (d_tile,))
        loop(n * n_d, body)

    def cols_of(ref, j):
        return ref[:, :, :, part_of(j, d_loc)].reshape(rows, d_loc)

    def add_wd(lo, n):
        def body(i):
            j, t = block_of(lo + i // n_ff), part_of(i % n_ff, ff_tile)
            acc_d[t] += dot(ha[part_of(j, rows), t], cols_of(gr, j), TN)
        loop(n * n_ff, body)

    def add_wup(acc, src, lo, n):
        def body(i):
            j, t = block_of(lo + i // n_ff), part_of(i % n_ff, ff_tile)
            acc[pl.ds(0, d_loc), t] += dot(cols_of(xr, j), src[part_of(j, rows), t], TN)
        loop(n * n_ff, body)

    n_buf = 8

    def units(part, k):
        bufs = [scat_bufs[(4 * k + u) * n_buf:(4 * k + u + 1) * n_buf] for u in range(4)]
        near = [Scatter(links, part, (0, 1, 2), True, bufs[0]), Scatter(links, part, (3, 4, 5), False, bufs[1])]
        return near, [Scatter(links, part, (6,), True, bufs[2]), Scatter(links, part, (7,), False, bufs[3])]

    y_near, y_far = units(y_part, 0)
    g_near, g_far = units(gx_part, 1)
    returns = []

    def finish(group, part, resid, stage, out):
        for unit in group:
            unit.end(1)
            for s in unit.slots:
                j = block_of(s)
                piece = (resid[j].astype(jnp.float32) + part[s, z, y]).astype(bf16)
                if s == 0:
                    out[:, part_of(dp, d_loc)] = piece
                else:
                    stage[s] = piece
        for unit in group:
            for s in unit.slots:
                if s:
                    returns.append(links.send(stage.at[s], out.at[:, part_of(dp, d_loc)], "block", block_of(s)))

    hid.forward()

    gather_end(cx)
    gather_end(cg)
    row_sends = [copy for rows_of in x_rows + g_rows for copy in rows_of.sent]
    for copy in row_sends:
        copy.wait_send()
    links.sent = [c for c in links.sent if not any(c is r for r in row_sends)]
    for j in range(N_DP):
        links.put(xc_ref.at[j], xr.at[:, :, :, pl.ds(j * d_loc, d_loc)])
        links.put(gc_ref.at[j], gr.at[:, :, :, pl.ds(j * d_loc, d_loc)])

    hid.near()
    y_blocks(0, 6)
    each(y_near, ("start", 0))
    dgate.forward()
    each(y_near, ("forward", 0))
    links.put_all()
    add_wd(0, 6)
    dgate.near()
    add_wup(acc_g, daa, 0, 6)
    dup.forward()
    each(y_near, ("end", 0), ("start", 1))
    dup.near()
    gx_blocks(0, 6)
    each(g_near, ("start", 0))
    hid.far()
    each(y_near, ("forward", 1))
    hid.near()
    y_blocks(6, 2)
    each(y_far, ("start", 0))
    each(g_near, ("forward", 0))
    add_wup(acc_u, dba, 0, 6)
    dgate.far()
    finish(y_near, y_part, xm, y_stage, y_ref)
    each(y_far, ("forward", 0))
    dup.far()
    dgate.near()
    dup.near()
    gx_blocks(6, 2)
    each(g_far, ("start", 0))
    add_wd(6, 2)
    links.put(acc_d, gwd_ref)
    each(g_near, ("end", 0), ("start", 1))
    add_wup(acc_g, daa, 6, 2)
    links.put(acc_g.at[pl.ds(0, d_loc)], gwg_ref)
    each(g_far, ("forward", 0))
    each(y_far, ("end", 0), ("start", 1))
    each(g_near, ("forward", 1))
    add_wup(acc_u, dba, 6, 2)
    links.put(acc_u.at[pl.ds(0, d_loc)], gwu_ref)
    each(g_far, ("end", 0), ("start", 1))
    each(y_far, ("forward", 1))
    each(g_far, ("forward", 1))
    finish(y_far, y_part, xm, y_stage, y_ref)
    finish(g_near, gx_part, gm, gx_stage, gx_ref)
    finish(g_far, gx_part, gm, gx_stage, gx_ref)
    gather_end(returns)
    links.sent_all()
    links.put_all()


PIECES = 4


def copy_kernel(*refs):
    n = (len(refs) - 2) // 3
    ins, outs, bufs, (in_sem, out_sem) = refs[:n], refs[n:2 * n], refs[2 * n:3 * n], refs[3 * n:]
    loads, stores = [], []
    for k in range(n):
        pieces = PIECES if ins[k].shape[0] >= 128 else 1
        size = ins[k].shape[0] // pieces
        for p in range(pieces):
            part, sem = pl.ds(p * size, size), k * PIECES + p
            loads.append(pltpu.make_async_copy(ins[k].at[part], bufs[k].at[part], in_sem.at[sem]))
            stores.append(pltpu.make_async_copy(bufs[k].at[part], outs[k].at[part], out_sem.at[sem]))
    for load in loads:
        load.start()
    for load, store in zip(loads, stores):
        load.wait()
        store.start()
    for store in stores:
        store.wait()


def solution(mesh):
    vmem = pl.BlockSpec(memory_space=VMEM)
    hbm = pl.BlockSpec(memory_space=pl.ANY)

    def local_step(x_loc, wg_loc, wu_loc, wd_loc, gy_loc):
        tok, d = x_loc.shape
        d_loc, ff = wg_loc.shape
        ffh = ff // 2
        bf16, f32 = x_loc.dtype, jnp.float32
        sds = jax.ShapeDtypeStruct
        n_sem = 240
        rows = RING * RING * tok
        spread = sds((N_DP, RING, RING, tok, d_loc), bf16)
        up_rows = max(d_loc, 2 * rows)
        whole = pltpu.VMEM((N_DP * rows, ff), bf16)
        mine = pltpu.VMEM((N_DP, tok, d_loc), bf16)
        scat = []
        for n in (3, 3, 1, 1):
            for half in ((n, 2, tok, d_loc), (n, tok, d_loc // 2)):
                scat += [pltpu.VMEM(half, f32)] * 2 + [pltpu.VMEM((2,) + half, f32)] * 2
        results = [sds((tok, d), bf16), sds((tok, d), bf16), sds((d_loc, ff), f32), sds((d_loc, ff), f32),
                   sds((ff, d_loc), f32)]
        outs = pl.pallas_call(
            mlp_kernel,
            out_shape=results + [spread, spread],
            in_specs=[vmem] * 2 + [hbm] * 3,
            out_specs=[vmem] * 2 + [hbm] * 5,
            scratch_shapes=[pltpu.VMEM((4 * d_loc, ffh), bf16)] * 4 + [pltpu.VMEM((ffh, 4 * d_loc), bf16)] * 2
            + [pltpu.VMEM((RING, RING, tok, SECTIONS * d_loc), bf16)] * 2 + [mine] * 2
            + [pltpu.VMEM((3, 2, rows, ffh), f32)] * 2 + [whole] * 3
            + [pltpu.VMEM((up_rows, ff), f32)] * 2 + [pltpu.VMEM((ff, d_loc), f32)]
            + [pltpu.VMEM((N_DP, RING, RING, tok, d_loc), f32)] * 2 + [mine] * 2 + scat * 2
            + [pltpu.SemaphoreType.DMA((n_sem,)), pltpu.SemaphoreType.DMA((n_sem,)), pltpu.SemaphoreType.DMA((32,))],
            compiler_params=pltpu.CompilerParams(collective_id=0, has_side_effects=True, vmem_limit_bytes=67043328),
            name="mlp",
        )(x_loc, gy_loc, wg_loc, wu_loc, wd_loc)[:5]
        return pl.pallas_call(
            copy_kernel,
            out_shape=results,
            in_specs=[hbm] * 5,
            out_specs=[hbm] * 5,
            scratch_shapes=[pltpu.VMEM(r.shape, r.dtype) for r in results]
            + [pltpu.SemaphoreType.DMA((5 * PIECES,))] * 2,
            name="results",
        )(*outs)

    row_spec = P(("dp", "tp"), None)
    up_spec = P("dp", "tp")
    down_spec = P("tp", "dp")
    return jax.shard_map(local_step, mesh=mesh,
                         in_specs=(row_spec, up_spec, up_spec, down_spec, row_spec),
                         out_specs=(row_spec, row_spec, up_spec, up_spec, down_spec),
                         check_vma=False)
```

```python
import itertools

import jax
import jax.numpy as jnp
from jax import lax
from jax.experimental import pallas as pl
from jax.experimental.pallas import tpu as pltpu
from jax.sharding import PartitionSpec as P

RING = 4
N_DP = 2 * RING
VMEM = pltpu.MemorySpace.VMEM


class Links:
    def __init__(self, send_sem, recv_sem, local_sem):
        self.send_sem, self.recv_sem, self.local_sem = send_sem, recv_sem, local_sem
        self.n_remote = self.n_local = 0
        self.sent, self.local = [], []
        dp, tp = lax.axis_index("dp"), lax.axis_index("tp")
        self.dp, self.tp = dp, tp
        self.x, self.core = dp // 2, dp % 2
        self.z, self.y = tp // RING, tp % RING
        odd = self.x % 2
        self.xa = self.x + 1 - 2 * odd
        self.xb = (self.x + 3 + 2 * odd) % RING

    def at(self, pos, off):
        return (pos + off) % RING

    def device(self, axis, off):
        if axis == "x":
            return {"dp": 2 * self.at(self.x, off) + self.core, "tp": self.tp}
        if axis == "a":
            return {"dp": 2 * self.xa + self.core, "tp": self.tp}
        if axis == "b":
            return {"dp": 2 * self.xb + self.core, "tp": self.tp}
        if axis == "block":
            return {"dp": off, "tp": self.tp}
        if axis == "core":
            return {"dp": 2 * self.x + (1 - self.core), "tp": self.tp}
        if axis == "dp":
            return {"dp": (self.dp + off) % N_DP, "tp": self.tp}
        if axis == "z":
            return {"dp": self.dp, "tp": RING * self.at(self.z, off) + self.y}
        return {"dp": self.dp, "tp": RING * self.z + self.at(self.y, off)}

    def barrier(self, peers):
        sem = pltpu.get_barrier_semaphore()
        for axis, off in peers:
            pl.semaphore_signal(sem, inc=1, device_id=self.device(axis, off),
                                device_id_type=pl.DeviceIdType.MESH)
        pl.semaphore_wait(sem, len(peers))

    def send(self, src, dst, axis, off=0):
        k = self.n_remote
        self.n_remote += 1
        copy = pltpu.make_async_remote_copy(
            src_ref=src, dst_ref=dst, send_sem=self.send_sem.at[k], recv_sem=self.recv_sem.at[k],
            device_id=self.device(axis, off), device_id_type=pl.DeviceIdType.MESH)
        copy.start()
        self.sent.append(copy)
        return copy

    def put(self, src, dst):
        k = self.n_local
        self.n_local += 1
        copy = pltpu.make_async_copy(src, dst, self.local_sem.at[k])
        copy.start()
        self.local.append(copy)
        return copy

    def sent_all(self):
        for copy in self.sent:
            copy.wait_send()
        self.sent = []

    def put_all(self):
        for copy in self.local:
            copy.wait()
        self.local = []


def gather_start(links, own, block, axis, pos):
    right = links.send(own, block(pos, None), axis, 1)
    left = links.send(own, block(pos, None), axis, -1)
    return right, left


def gather_forward(links, copies, block, axis, pos):
    copies[0].wait_recv()
    from_left = links.at(pos, -1)
    right = links.send(block(from_left, 0), block(from_left, 0), axis, 1)
    copies[1].wait_recv()
    from_right = links.at(pos, 1)
    left = links.send(block(from_right, 1), block(from_right, 1), axis, -1)
    return right, left


def gather_end(copies):
    for copy in copies:
        copy.wait_recv()


class DpGather:
    def __init__(self, links, own, slot):
        self.links, self.slot = links, slot
        x, c = links.x, links.core
        self.block = lambda p, h: slot(2 * p + c, h)
        self.ring = gather_start(links, own, self.block, "x", x)
        self.mate = [links.send(own, slot(links.dp, None), "core")]

    def forward(self):
        links = self.links
        self.ring = gather_forward(links, self.ring, self.block, "x", links.x)
        for off in (-1, 1):
            b = self.block(links.at(links.x, off), None)
            self.mate.append(links.send(b, b, "core"))

    def own(self):
        gather_end(self.mate[:1])
        self.mate = self.mate[1:]

    def near(self):
        gather_end(self.mate)
        self.mate = []

    def far(self):
        links = self.links
        far = links.at(links.x, 2)
        for h in (0, 1):
            self.ring[h].wait_recv()
            b = self.block(far, h)
            self.mate.append(links.send(b, b, "core"))


class PairGather:
    def __init__(self, links, own, slots):
        self.links, self.slots = links, slots
        c = links.core
        self.pair = [links.send(own(h), slots[h](2 + c), "ab"[h]) for h in (0, 1)]
        self.mate = [links.send(own(h), slots[h](c), "core") for h in (0, 1)]
        for h in (0, 1):
            links.put(own(h), slots[h](c))

    def forward(self):
        links = self.links
        for h in (0, 1):
            self.pair[h].wait_recv()
            s = self.slots[h](2 + links.core)
            self.mate.append(links.send(s, s, "core"))

    def near(self):
        gather_end(self.mate)


class Rows:
    def __init__(self, links, ref, lo, width, z_first):
        self.links, z, y = links, links.z, links.y
        half = width // 2
        cols = pl.ds(lo, width)
        if z_first:
            self.axes, self.pos = ("z", "y"), (z, y)
            first = lambda p, h: ref.at[p, y, :, cols if h is None else pl.ds(lo + h * half, half)]
            second = lambda p, h: ref.at[slice(None) if h is None else pl.ds(2 * h, 2), p, :, cols]
        else:
            self.axes, self.pos = ("y", "z"), (y, z)
            first = lambda p, h: ref.at[z, p, :, cols if h is None else pl.ds(lo + h * half, half)]
            second = lambda p, h: ref.at[p, slice(None) if h is None else pl.ds(2 * h, 2), :, cols]
        self.block = (first, second)
        self.sent = []

    def start(self, phase):
        block, pos = self.block[phase], self.pos[phase]
        self.copies = gather_start(self.links, block(pos, None), block, self.axes[phase], pos)
        self.sent.extend(self.copies)

    def forward(self, phase):
        self.copies = gather_forward(self.links, self.copies, self.block[phase], self.axes[phase], self.pos[phase])
        self.sent.extend(self.copies)

    def end(self, phase):
        gather_end(self.copies)


class Scatter:
    def __init__(self, links, part, slots, z_first, bufs):
        self.links, z, y = links, links.z, links.y
        half = part.shape[-1] // 2
        self.slots = slots
        n = pl.ds(slots[0], len(slots))
        if z_first:
            self.axes, self.pos = ("z", "y"), (z, y)
            first = lambda p, h: part.at[n, p, pl.ds(2 * h, 2)]
            second = lambda p, h: part.at[n, z, p, :, pl.ds(h * half, half)]
        else:
            self.axes, self.pos = ("y", "z"), (y, z)
            first = lambda p, h: part.at[n, pl.ds(2 * h, 2), p]
            second = lambda p, h: part.at[n, p, y, :, pl.ds(h * half, half)]
        self.block = (first, second)
        self.bufs = (bufs[:4], bufs[4:])

    def start(self, phase):
        links, block, axis, pos = self.links, self.block[phase], self.axes[phase], self.pos[phase]
        near0, near1, l_ref, r_ref = self.bufs[phase]
        far = links.at(pos, 2)
        self.first = (links.send(block(far, 0), near0, axis, 1), links.send(block(far, 1), near1, axis, -1))
        self.last = [links.send(block(links.at(pos, 1), 1), l_ref.at[1], axis, 1),
                     links.send(block(links.at(pos, -1), 0), r_ref.at[0], axis, -1)]

    def forward(self, phase):
        links, block, axis, pos = self.links, self.block[phase], self.axes[phase], self.pos[phase]
        near0, near1, l_ref, r_ref = self.bufs[phase]
        for copy, off, h, near, dst in ((self.first[0], 1, 0, near0, l_ref), (self.first[1], -1, 1, near1, r_ref)):
            copy.wait_recv()
            b = block(links.at(pos, off), h)
            add_into(b, [near])
            self.last.append(links.send(b, dst.at[h], axis, off))

    def end(self, phase):
        block, pos = self.block[phase], self.pos[phase]
        _, _, l_ref, r_ref = self.bufs[phase]
        gather_end(self.last)
        for h in (0, 1):
            add_into(block(pos, h), [l_ref.at[h], r_ref.at[h]])


TILE = 256


def add_into(dst, terms):
    for lead in itertools.product(*(range(n) for n in dst.shape[:-2])):
        total = dst[lead]
        for t in terms:
            total = total + t[lead]
        dst[lead] = total


def loop(n, body):
    def step(i, carry):
        body(i)
        return carry
    lax.fori_loop(0, n, step, 0)


def part_of(i, size):
    return pl.ds(pl.multiple_of(i * size, size), size)


NN = (((1,), (0,)), ((), ()))
NT = (((1,), (1,)), ((), ()))
TN = (((0,), (0,)), ((), ()))


def dot(a, b, dims):
    return lax.dot_general(a, b, dims, preferred_element_type=jnp.float32)


OWN, OWN_A, OWN_B, TOK_B, TOK_A, SECTIONS = 0, 2, 4, 6, 10, 14


def mlp_kernel(x_ref, gy_ref, wg_ref, wu_ref, wd_ref,
               y_ref, gx_ref, gwg_ref, gwu_ref, gwd_ref, xc_ref, gc_ref,
               wga, wgb, wua, wub, wda, wdb, xr, gr, xm, gm, q_out, q_in, ha, daa, dba,
               acc_g, acc_u, acc_d, y_part, gx_part, y_stage, gx_stage, *rest):
    scat_bufs, (send_sem, recv_sem, local_sem) = rest[:-3], rest[-3:]
    links = Links(send_sem, recv_sem, local_sem)
    dp, z, y, x, core = links.dp, links.z, links.y, links.x, links.core
    tok, d = x_ref.shape
    d_loc, ff = wg_ref.shape
    ffh = ff // 2
    rows = RING * RING * tok
    bf16 = x_ref.dtype
    links.barrier([("dp", o) for o in range(1, N_DP)] + [("z", 1), ("z", -1), ("y", 1), ("y", -1)])

    def d_of(ref, j, n=1):
        return ref.at[:, part_of(j, n * d_loc)]

    def section(ref, s, n):
        return ref.at[z, y, :, pl.ds(s * d_loc, n * d_loc)]

    def spread(src, dst):
        return [links.send(d_of(src, (dp + o) % N_DP), dst.at[dp], "dp", o) for o in range(1, N_DP)]

    opp = links.at(x, 2)

    def lend(src, dst):
        return [links.send(d_of(src, links.xb, 2), section(dst, TOK_B, 2), "b"),
                links.send(d_of(src, opp, 2), section(dst, TOK_B + 2, 2), "b"),
                links.send(d_of(src, links.xa, 2), section(dst, TOK_A, 2), "a"),
                links.send(d_of(src, opp, 2), section(dst, TOK_A + 2, 2), "a")]

    lent = [lend(x_ref, xr), lend(gy_ref, gr)]
    gate = PairGather(links, lambda h: wg_ref.at[:, pl.ds(h * ffh, ffh)],
                      [lambda k: wga.at[part_of(k, d_loc)], lambda k: wgb.at[part_of(k, d_loc)]])
    up = PairGather(links, lambda h: wu_ref.at[:, pl.ds(h * ffh, ffh)],
                    [lambda k: wua.at[part_of(k, d_loc)], lambda k: wub.at[part_of(k, d_loc)]])
    spreads = [spread(x_ref, xm), spread(gy_ref, gm)]
    down = PairGather(links, lambda h: wd_ref.at[pl.ds(h * ffh, ffh)],
                      [lambda k: wda.at[:, part_of(k, d_loc)], lambda k: wdb.at[:, part_of(k, d_loc)]])
    for src, dst, mine in ((x_ref, xr, xm), (gy_ref, gr, gm)):
        for s, j in ((OWN, x), (OWN_A, links.xa), (OWN_B, links.xb)):
            dst[z, y, :, s * d_loc:(s + 2) * d_loc] = src[:, part_of(j, 2 * d_loc)]
        mine[dp] = src[:, part_of(dp, d_loc)]

    def each(group, *steps):
        for name, phase in steps:
            for unit in group:
                getattr(unit, name)(phase)

    row_half = SECTIONS * d_loc // 2
    x_rows = [Rows(links, xr, 0, row_half, True), Rows(links, xr, row_half, row_half, False)]
    g_rows = [Rows(links, gr, 0, row_half, True), Rows(links, gr, row_half, row_half, False)]

    def dp_half(h):
        return pl.ds(h * (N_DP // 2), N_DP // 2)

    def xc_first(p, h):
        return xc_ref.at[:, p, y] if h is None else xc_ref.at[dp_half(h), p, y]

    def xc_second(p, h):
        return xc_ref.at[:, :, p] if h is None else xc_ref.at[dp_half(h), :, p]

    def gc_first(p, h):
        return gc_ref.at[:, z, p] if h is None else gc_ref.at[dp_half(h), z, p]

    def gc_second(p, h):
        return gc_ref.at[:, p] if h is None else gc_ref.at[dp_half(h), p]

    gather_end(lent[0])
    each(x_rows, ("start", 0))
    gather_end(lent[1])
    each(x_rows, ("forward", 0), ("end", 0), ("start", 1))
    each(g_rows, ("start", 0))
    each(x_rows, ("forward", 1))
    links.put_all()
    gate.forward()
    each(g_rows, ("forward", 0), ("end", 0), ("start", 1))
    each(x_rows, ("end", 1))

    accs = (acc_g.at[pl.ds(0, rows)], acc_g.at[pl.ds(rows, rows)], acc_u.at[pl.ds(0, rows)])
    tile = min(TILE, ffh)
    n_tile = ffh // tile

    def take(ref, s, n):
        return ref[:, :, :, s * d_loc:(s + n) * d_loc].reshape(rows, n * d_loc)

    def product(src, s, n, w, first, t, down_side):
        if down_side:
            return dot(take(src, s, n), w[t, first * d_loc:(first + n) * d_loc], NT)
        return dot(take(src, s, n), w[first * d_loc:(first + n) * d_loc, t], NN)

    def lend_sums(k, src, wa, wb, down_side):
        def body(i):
            t = part_of(i, tile)
            q_out[k, 0, :, t] = product(src, TOK_B, 4, wa, 0, t, down_side)
            q_out[k, 1, :, t] = product(src, TOK_A, 4, wb, 0, t, down_side)
        loop(n_tile, body)
        return [links.send(q_out.at[k, 0], q_in.at[k, 0], "b"), links.send(q_out.at[k, 1], q_in.at[k, 1], "a")]

    def own_sums(k, src, wa, wb, down_side):
        def body(i):
            t = part_of(i, tile)
            accs[k][:, t] = product(src, OWN, 4, wa, 0, t, down_side)
            accs[k][:, part_of(i + n_tile, tile)] = (product(src, OWN, 2, wb, 0, t, down_side)
                                                     + product(src, OWN_B, 2, wb, 2, t, down_side))
        loop(n_tile, body)

    gate.near()
    qa = lend_sums(0, xr, wga, wgb, False)
    up.forward()
    up.near()
    qb = lend_sums(1, xr, wua, wub, False)
    for copies in spreads:
        gather_end(copies)
    links.put(xm, xc_first(z, None))
    links.put(gm, gc_first(y, None))
    each(g_rows, ("forward", 1))
    cx = gather_start(links, xm, xc_first, "z", z)
    cg = gather_start(links, gm, gc_first, "y", y)
    own_sums(0, xr, wga, wgb, False)
    own_sums(1, xr, wua, wub, False)
    down.forward()
    each(g_rows, ("end", 1))
    down.near()
    qg = lend_sums(2, gr, wda, wdb, True)
    cx = gather_forward(links, cx, xc_first, "z", z)
    cg = gather_forward(links, cg, gc_first, "y", y)
    own_sums(2, gr, wda, wdb, True)
    links.put_all()

    step_rows = 16

    def gate_loop(body):
        def step(i):
            r = part_of(i, step_rows)
            own = part_of(dp * (rows // step_rows) + i, step_rows)
            for h in (0, 1):
                cols = pl.ds(h * ffh, ffh)
                body(own, cols, lambda k: accs[k][r, cols] + q_in[k, h, r])
        loop(rows // step_rows, step)

    def hidden_body(own, cols, value):
        a = value(0)
        ha[own, cols] = (a * jax.nn.sigmoid(a) * value(1)).astype(bf16)

    gather_end(qa)
    gather_end(qb)
    gate_loop(hidden_body)
    mine = part_of(dp, rows)

    def row_slot(ref):
        def slot(j, h):
            if h is None:
                return ref.at[part_of(j, rows)]
            return ref.at[part_of(2 * j + h, rows // 2)]
        return slot

    hid = DpGather(links, ha.at[mine], row_slot(ha))
    gather_end(cx)
    cx = gather_start(links, xc_second(y, None), xc_second, "y", y)
    gather_end(cg)
    cg = gather_start(links, gc_second(z, None), gc_second, "z", z)

    def grad_body(own, cols, value):
        a, g = value(0), value(2)
        s = jax.nn.sigmoid(a)
        daa[own, cols] = (g * value(1) * (s * (1.0 + a * (1.0 - s)))).astype(bf16)
        dba[own, cols] = (g * (a * s)).astype(bf16)

    gather_end(qg)
    gate_loop(grad_body)
    dgate = DpGather(links, daa.at[mine], row_slot(daa))
    dup = DpGather(links, dba.at[mine], row_slot(dba))

    cx = gather_forward(links, cx, xc_second, "y", y)
    cg = gather_forward(links, cg, gc_second, "z", z)

    def clear(*refs):
        for ref in refs:
            n, step = ref.shape[0], min(16, ref.shape[0])

            def body(i):
                ref[part_of(i, step)] = jnp.zeros((step, ref.shape[1]), jnp.float32)
            loop(n // step, body)

    clear(acc_g, acc_u, acc_d)

    def block_of(s):
        p = s // 2
        return 2 * ((x + p + p // 2 - 2 * (p // 3)) % RING) + (core + s) % 2

    d_tile = min(TILE, d_loc)
    n_d = d_loc // d_tile
    ff_tile = min(TILE, ff)
    n_ff = ff // ff_tile
    low, high = pl.ds(0, ffh), pl.ds(ffh, ffh)
    torus = (RING, RING, tok)

    def y_blocks(lo, n):
        def body(i):
            s = lo + i // n_d
            r, t = part_of(block_of(s), rows), part_of(i % n_d, d_tile)
            w = part_of(core * n_d + i % n_d, d_tile)
            y_part[s, :, :, :, t] = (dot(ha[r, low], wda[:, w], NN) + dot(ha[r, high], wdb[:, w], NN)).reshape(
                torus + (d_tile,))
        loop(n * n_d, body)

    def gx_blocks(lo, n):
        def body(i):
            s = lo + i // n_d
            r, t = part_of(block_of(s), rows), part_of(i % n_d, d_tile)
            w = part_of(core * n_d + i % n_d, d_tile)
            gx_part[s, :, :, :, t] = (dot(daa[r, low], wga[w], NT) + dot(daa[r, high], wgb[w], NT)
                                      + dot(dba[r, low], wua[w], NT) + dot(dba[r, high], wub[w], NT)).reshape(
                torus + (d_tile,))
        loop(n * n_d, body)

    def cols_of(ref, j):
        return ref[:, :, :, part_of(j, d_loc)].reshape(rows, d_loc)

    def add_wd(lo, n):
        def body(i):
            j, t = block_of(lo + i // n_ff), part_of(i % n_ff, ff_tile)
            acc_d[t] += dot(ha[part_of(j, rows), t], cols_of(gr, j), TN)
        loop(n * n_ff, body)

    def add_wup(acc, src, lo, n):
        def body(i):
            j, t = block_of(lo + i // n_ff), part_of(i % n_ff, ff_tile)
            acc[pl.ds(0, d_loc), t] += dot(cols_of(xr, j), src[part_of(j, rows), t], TN)
        loop(n * n_ff, body)

    n_buf = 8
    groups = ((0,), (1,)), ((2, 3), (4, 5)), ((6,), (7,))

    def units(part, k):
        bufs = [scat_bufs[(6 * k + u) * n_buf:(6 * k + u + 1) * n_buf] for u in range(6)]
        return [[Scatter(links, part, pair[i], i == 0, bufs[2 * n + i]) for i in (0, 1)]
                for n, pair in enumerate(groups)]

    y_own, y_near, y_far = units(y_part, 0)
    g_own, g_near, g_far = units(gx_part, 1)
    returns = []

    def finish(group, part, resid, stage, out):
        for unit in group:
            unit.end(1)
            for s in unit.slots:
                j = block_of(s)
                piece = (resid[j].astype(jnp.float32) + part[s, z, y]).astype(bf16)
                if s == 0:
                    out[:, part_of(dp, d_loc)] = piece
                else:
                    stage[s] = piece
        for unit in group:
            for s in unit.slots:
                if s:
                    returns.append(links.send(stage.at[s], out.at[:, part_of(dp, d_loc)], "block", block_of(s)))

    for gathered in (hid, dgate, dup):
        gathered.own()
    y_blocks(0, 2)
    each(y_own, ("start", 0))
    each(y_own, ("forward", 0))
    hid.forward()
    hid.near()
    y_blocks(2, 4)
    each(y_near, ("start", 0))
    gather_end(cx)
    gather_end(cg)
    row_sends = [copy for rows_of in x_rows + g_rows for copy in rows_of.sent]
    for copy in row_sends:
        copy.wait_send()
    links.sent = [c for c in links.sent if not any(c is r for r in row_sends)]
    for j in range(N_DP):
        links.put(xc_ref.at[j], xr.at[:, :, :, pl.ds(j * d_loc, d_loc)])
        links.put(gc_ref.at[j], gr.at[:, :, :, pl.ds(j * d_loc, d_loc)])
    gx_blocks(0, 2)
    each(g_own, ("start", 0))
    dgate.forward()
    links.put_all()
    add_wd(0, 6)
    each(y_near, ("forward", 0))
    dgate.near()
    add_wup(acc_g, daa, 0, 6)
    each(y_near, ("end", 0), ("start", 1))
    each(y_own, ("end", 0), ("start", 1))
    dup.forward()
    each(g_own, ("forward", 0))
    each(y_near, ("forward", 1))
    dup.near()
    gx_blocks(2, 4)
    each(g_near, ("start", 0))
    hid.far()
    add_wup(acc_u, dba, 0, 6)
    hid.near()
    each(g_own, ("end", 0), ("start", 1))
    y_blocks(6, 2)
    each(y_far, ("start", 0))
    each(g_near, ("forward", 0))
    finish(y_near, y_part, xm, y_stage, y_ref)
    each(y_own, ("forward", 1))
    add_wd(6, 2)
    links.put(acc_d, gwd_ref)
    each(g_own, ("forward", 1))
    dgate.far()
    each(y_far, ("forward", 0))
    dgate.near()
    dup.far()
    dup.near()
    gx_blocks(6, 2)
    each(g_far, ("start", 0))
    add_wup(acc_g, daa, 6, 2)
    links.put(acc_g.at[pl.ds(0, d_loc)], gwg_ref)
    each(y_far, ("end", 0), ("start", 1))
    finish(y_own, y_part, xm, y_stage, y_ref)
    each(g_far, ("forward", 0))
    each(y_far, ("forward", 1))
    each(g_near, ("end", 0), ("start", 1))
    each(g_far, ("end", 0), ("start", 1))
    finish(y_far, y_part, xm, y_stage, y_ref)
    each(g_near, ("forward", 1))
    each(g_far, ("forward", 1))
    finish(g_own, gx_part, gm, gx_stage, gx_ref)
    finish(g_near, gx_part, gm, gx_stage, gx_ref)
    finish(g_far, gx_part, gm, gx_stage, gx_ref)
    add_wup(acc_u, dba, 6, 2)
    links.put(acc_u.at[pl.ds(0, d_loc)], gwu_ref)
    gather_end(returns)
    links.sent_all()
    links.put_all()


PIECES = 4


def copy_kernel(*refs):
    n = (len(refs) - 2) // 3
    ins, outs, bufs, (in_sem, out_sem) = refs[:n], refs[n:2 * n], refs[2 * n:3 * n], refs[3 * n:]
    loads, stores = [], []
    for k in range(n):
        pieces = PIECES if ins[k].shape[0] >= 128 else 1
        size = ins[k].shape[0] // pieces
        for p in range(pieces):
            part, sem = pl.ds(p * size, size), k * PIECES + p
            loads.append(pltpu.make_async_copy(ins[k].at[part], bufs[k].at[part], in_sem.at[sem]))
            stores.append(pltpu.make_async_copy(bufs[k].at[part], outs[k].at[part], out_sem.at[sem]))
    for load in loads:
        load.start()
    for load, store in zip(loads, stores):
        load.wait()
        store.start()
    for store in stores:
        store.wait()


def solution(mesh):
    vmem = pl.BlockSpec(memory_space=VMEM)
    hbm = pl.BlockSpec(memory_space=pl.ANY)

    def local_step(x_loc, wg_loc, wu_loc, wd_loc, gy_loc):
        tok, d = x_loc.shape
        d_loc, ff = wg_loc.shape
        ffh = ff // 2
        bf16, f32 = x_loc.dtype, jnp.float32
        sds = jax.ShapeDtypeStruct
        n_sem = 288
        rows = RING * RING * tok
        spread = sds((N_DP, RING, RING, tok, d_loc), bf16)
        up_rows = max(d_loc, 2 * rows)
        whole = pltpu.VMEM((N_DP * rows, ff), bf16)
        mine = pltpu.VMEM((N_DP, tok, d_loc), bf16)
        scat = []
        for n in (1, 1, 2, 2, 1, 1):
            for half in ((n, 2, tok, d_loc), (n, tok, d_loc // 2)):
                scat += [pltpu.VMEM(half, f32)] * 2 + [pltpu.VMEM((2,) + half, f32)] * 2
        results = [sds((tok, d), bf16), sds((tok, d), bf16), sds((d_loc, ff), f32), sds((d_loc, ff), f32),
                   sds((ff, d_loc), f32)]
        outs = pl.pallas_call(
            mlp_kernel,
            out_shape=results + [spread, spread],
            in_specs=[vmem] * 2 + [hbm] * 3,
            out_specs=[vmem] * 2 + [hbm] * 5,
            scratch_shapes=[pltpu.VMEM((4 * d_loc, ffh), bf16)] * 4 + [pltpu.VMEM((ffh, 4 * d_loc), bf16)] * 2
            + [pltpu.VMEM((RING, RING, tok, SECTIONS * d_loc), bf16)] * 2 + [mine] * 2
            + [pltpu.VMEM((3, 2, rows, ffh), f32)] * 2 + [whole] * 3
            + [pltpu.VMEM((up_rows, ff), f32)] * 2 + [pltpu.VMEM((ff, d_loc), f32)]
            + [pltpu.VMEM((N_DP, RING, RING, tok, d_loc), f32)] * 2 + [mine] * 2 + scat * 2
            + [pltpu.SemaphoreType.DMA((n_sem,)), pltpu.SemaphoreType.DMA((n_sem,)), pltpu.SemaphoreType.DMA((32,))],
            compiler_params=pltpu.CompilerParams(collective_id=0, has_side_effects=True, vmem_limit_bytes=67043328),
            name="mlp",
        )(x_loc, gy_loc, wg_loc, wu_loc, wd_loc)[:5]
        return pl.pallas_call(
            copy_kernel,
            out_shape=results,
            in_specs=[hbm] * 5,
            out_specs=[hbm] * 5,
            scratch_shapes=[pltpu.VMEM(r.shape, r.dtype) for r in results]
            + [pltpu.SemaphoreType.DMA((5 * PIECES,))] * 2,
            name="results",
        )(*outs)

    row_spec = P(("dp", "tp"), None)
    up_spec = P("dp", "tp")
    down_spec = P("tp", "dp")
    return jax.shard_map(local_step, mesh=mesh,
                         in_specs=(row_spec, up_spec, up_spec, down_spec, row_spec),
                         out_specs=(row_spec, row_spec, up_spec, up_spec, down_spec),
                         check_vma=False)
```

```python
import itertools

import jax
import jax.numpy as jnp
from jax import lax
from jax.experimental import pallas as pl
from jax.experimental.pallas import tpu as pltpu
from jax.sharding import PartitionSpec as P

RING = 4
N_DP = 2 * RING
VMEM = pltpu.MemorySpace.VMEM


class Links:
    def __init__(self, send_sem, recv_sem, local_sem):
        self.send_sem, self.recv_sem, self.local_sem = send_sem, recv_sem, local_sem
        self.n_remote = self.n_local = 0
        self.sent, self.local = [], []
        dp, tp = lax.axis_index("dp"), lax.axis_index("tp")
        self.dp, self.tp = dp, tp
        self.x, self.core = dp // 2, dp % 2
        self.z, self.y = tp // RING, tp % RING
        odd = self.x % 2
        self.xa = self.x + 1 - 2 * odd
        self.xb = (self.x + 3 + 2 * odd) % RING

    def at(self, pos, off):
        return (pos + off) % RING

    def device(self, axis, off):
        if axis == "x":
            return {"dp": 2 * self.at(self.x, off) + self.core, "tp": self.tp}
        if axis == "a":
            return {"dp": 2 * self.xa + self.core, "tp": self.tp}
        if axis == "b":
            return {"dp": 2 * self.xb + self.core, "tp": self.tp}
        if axis == "block":
            return {"dp": off, "tp": self.tp}
        if axis == "core":
            return {"dp": 2 * self.x + (1 - self.core), "tp": self.tp}
        if axis == "dp":
            return {"dp": (self.dp + off) % N_DP, "tp": self.tp}
        if axis == "z":
            return {"dp": self.dp, "tp": RING * self.at(self.z, off) + self.y}
        return {"dp": self.dp, "tp": RING * self.z + self.at(self.y, off)}

    def barrier(self, peers):
        sem = pltpu.get_barrier_semaphore()
        for axis, off in peers:
            pl.semaphore_signal(sem, inc=1, device_id=self.device(axis, off),
                                device_id_type=pl.DeviceIdType.MESH)
        pl.semaphore_wait(sem, len(peers))

    def send(self, src, dst, axis, off=0):
        k = self.n_remote
        self.n_remote += 1
        copy = pltpu.make_async_remote_copy(
            src_ref=src, dst_ref=dst, send_sem=self.send_sem.at[k], recv_sem=self.recv_sem.at[k],
            device_id=self.device(axis, off), device_id_type=pl.DeviceIdType.MESH)
        copy.start()
        self.sent.append(copy)
        return copy

    def put(self, src, dst):
        k = self.n_local
        self.n_local += 1
        copy = pltpu.make_async_copy(src, dst, self.local_sem.at[k])
        copy.start()
        self.local.append(copy)
        return copy

    def sent_all(self):
        for copy in self.sent:
            copy.wait_send()
        self.sent = []

    def put_all(self):
        for copy in self.local:
            copy.wait()
        self.local = []


def gather_start(links, own, block, axis, pos):
    right = links.send(own, block(pos, None), axis, 1)
    left = links.send(own, block(pos, None), axis, -1)
    return right, left


def gather_forward(links, copies, block, axis, pos):
    copies[0].wait_recv()
    from_left = links.at(pos, -1)
    right = links.send(block(from_left, 0), block(from_left, 0), axis, 1)
    copies[1].wait_recv()
    from_right = links.at(pos, 1)
    left = links.send(block(from_right, 1), block(from_right, 1), axis, -1)
    return right, left


def gather_end(copies):
    for copy in copies:
        copy.wait_recv()


class DpGather:
    def __init__(self, links, own, slot):
        self.links, self.slot = links, slot
        x, c = links.x, links.core
        self.block = lambda p, h: slot(2 * p + c, h)
        self.ring = gather_start(links, own, self.block, "x", x)
        self.mate = [links.send(own, slot(links.dp, None), "core")]

    def forward(self):
        links = self.links
        self.ring = gather_forward(links, self.ring, self.block, "x", links.x)
        for off in (-1, 1):
            b = self.block(links.at(links.x, off), None)
            self.mate.append(links.send(b, b, "core"))

    def own(self):
        gather_end(self.mate[:1])
        self.mate = self.mate[1:]

    def near(self):
        gather_end(self.mate)
        self.mate = []

    def far(self):
        links = self.links
        far = links.at(links.x, 2)
        for h in (0, 1):
            self.ring[h].wait_recv()
            b = self.block(far, h)
            self.mate.append(links.send(b, b, "core"))


class PairGather:
    def __init__(self, links, own, slots):
        self.links, self.slots = links, slots
        c = links.core
        self.pair = [links.send(own(h), slots[h](2 + c), "ab"[h]) for h in (0, 1)]
        self.mate = [links.send(own(h), slots[h](c), "core") for h in (0, 1)]
        for h in (0, 1):
            links.put(own(h), slots[h](c))

    def forward(self):
        links = self.links
        for h in (0, 1):
            self.pair[h].wait_recv()
            s = self.slots[h](2 + links.core)
            self.mate.append(links.send(s, s, "core"))

    def near(self):
        gather_end(self.mate)


class Rows:
    def __init__(self, links, ref, lo, width, z_first):
        self.links, z, y = links, links.z, links.y
        half = width // 2
        cols = pl.ds(lo, width)
        if z_first:
            self.axes, self.pos = ("z", "y"), (z, y)
            first = lambda p, h: ref.at[p, y, :, cols if h is None else pl.ds(lo + h * half, half)]
            second = lambda p, h: ref.at[slice(None) if h is None else pl.ds(2 * h, 2), p, :, cols]
        else:
            self.axes, self.pos = ("y", "z"), (y, z)
            first = lambda p, h: ref.at[z, p, :, cols if h is None else pl.ds(lo + h * half, half)]
            second = lambda p, h: ref.at[p, slice(None) if h is None else pl.ds(2 * h, 2), :, cols]
        self.block = (first, second)
        self.sent = []

    def start(self, phase):
        block, pos = self.block[phase], self.pos[phase]
        self.copies = gather_start(self.links, block(pos, None), block, self.axes[phase], pos)
        self.sent.extend(self.copies)

    def forward(self, phase):
        self.copies = gather_forward(self.links, self.copies, self.block[phase], self.axes[phase], self.pos[phase])
        self.sent.extend(self.copies)

    def end(self, phase):
        gather_end(self.copies)


class Scatter:
    def __init__(self, links, part, slots, z_first, bufs):
        self.links, z, y = links, links.z, links.y
        half = part.shape[-1] // 2
        self.slots = slots
        n = pl.ds(slots[0], len(slots))
        if z_first:
            self.axes, self.pos = ("z", "y"), (z, y)
            first = lambda p, h: part.at[n, p, pl.ds(2 * h, 2)]
            second = lambda p, h: part.at[n, z, p, :, pl.ds(h * half, half)]
        else:
            self.axes, self.pos = ("y", "z"), (y, z)
            first = lambda p, h: part.at[n, pl.ds(2 * h, 2), p]
            second = lambda p, h: part.at[n, p, y, :, pl.ds(h * half, half)]
        self.block = (first, second)
        self.bufs = (bufs[:4], bufs[4:])

    def start(self, phase):
        links, block, axis, pos = self.links, self.block[phase], self.axes[phase], self.pos[phase]
        near0, near1, l_ref, r_ref = self.bufs[phase]
        far = links.at(pos, 2)
        self.first = (links.send(block(far, 0), near0, axis, 1), links.send(block(far, 1), near1, axis, -1))
        self.last = [links.send(block(links.at(pos, 1), 1), l_ref.at[1], axis, 1),
                     links.send(block(links.at(pos, -1), 0), r_ref.at[0], axis, -1)]

    def forward(self, phase):
        links, block, axis, pos = self.links, self.block[phase], self.axes[phase], self.pos[phase]
        near0, near1, l_ref, r_ref = self.bufs[phase]
        for copy, off, h, near, dst in ((self.first[0], 1, 0, near0, l_ref), (self.first[1], -1, 1, near1, r_ref)):
            copy.wait_recv()
            b = block(links.at(pos, off), h)
            add_into(b, [near])
            self.last.append(links.send(b, dst.at[h], axis, off))

    def end(self, phase):
        block, pos = self.block[phase], self.pos[phase]
        _, _, l_ref, r_ref = self.bufs[phase]
        gather_end(self.last)
        for h in (0, 1):
            add_into(block(pos, h), [l_ref.at[h], r_ref.at[h]])


TILE = 256


def add_into(dst, terms):
    for lead in itertools.product(*(range(n) for n in dst.shape[:-2])):
        total = dst[lead]
        for t in terms:
            total = total + t[lead]
        dst[lead] = total


def loop(n, body):
    def step(i, carry):
        body(i)
        return carry
    lax.fori_loop(0, n, step, 0)


def part_of(i, size):
    return pl.ds(pl.multiple_of(i * size, size), size)


NN = (((1,), (0,)), ((), ()))
NT = (((1,), (1,)), ((), ()))
TN = (((0,), (0,)), ((), ()))


def dot(a, b, dims):
    return lax.dot_general(a, b, dims, preferred_element_type=jnp.float32)


OWN, OWN_A, OWN_B, TOK_B, TOK_A, SECTIONS = 0, 2, 4, 6, 10, 14


def mlp_kernel(x_ref, gy_ref, wg_ref, wu_ref, wd_ref,
               y_ref, gx_ref, acc_g, acc_u, acc_d, xc_ref, gc_ref,
               wga, wgb, wua, wub, wda, wdb, xr, gr, xm, gm, q_out, q_in, ha, daa, dba,
               y_part, gx_part, y_stage, gx_stage, *rest):
    scat_bufs, (send_sem, recv_sem, local_sem) = rest[:-3], rest[-3:]
    links = Links(send_sem, recv_sem, local_sem)
    dp, z, y, x, core = links.dp, links.z, links.y, links.x, links.core
    tok, d = x_ref.shape
    d_loc, ff = wg_ref.shape
    ffh = ff // 2
    rows = RING * RING * tok
    bf16 = x_ref.dtype
    links.barrier([("dp", o) for o in range(1, N_DP)] + [("z", 1), ("z", -1), ("y", 1), ("y", -1)])

    def d_of(ref, j, n=1):
        return ref.at[:, part_of(j, n * d_loc)]

    def section(ref, s, n):
        return ref.at[z, y, :, pl.ds(s * d_loc, n * d_loc)]

    def spread(src, dst):
        return [links.send(d_of(src, (dp + o) % N_DP), dst.at[dp], "dp", o) for o in range(1, N_DP)]

    opp = links.at(x, 2)

    def lend(src, dst):
        return [links.send(d_of(src, links.xb, 2), section(dst, TOK_B, 2), "b"),
                links.send(d_of(src, opp, 2), section(dst, TOK_B + 2, 2), "b"),
                links.send(d_of(src, links.xa, 2), section(dst, TOK_A, 2), "a"),
                links.send(d_of(src, opp, 2), section(dst, TOK_A + 2, 2), "a")]

    lent = [lend(x_ref, xr), lend(gy_ref, gr)]
    gate = PairGather(links, lambda h: wg_ref.at[:, pl.ds(h * ffh, ffh)],
                      [lambda k: wga.at[part_of(k, d_loc)], lambda k: wgb.at[part_of(k, d_loc)]])
    up = PairGather(links, lambda h: wu_ref.at[:, pl.ds(h * ffh, ffh)],
                    [lambda k: wua.at[part_of(k, d_loc)], lambda k: wub.at[part_of(k, d_loc)]])
    spreads = [spread(x_ref, xm), spread(gy_ref, gm)]
    down = PairGather(links, lambda h: wd_ref.at[pl.ds(h * ffh, ffh)],
                      [lambda k: wda.at[:, part_of(k, d_loc)], lambda k: wdb.at[:, part_of(k, d_loc)]])
    for src, dst, mine in ((x_ref, xr, xm), (gy_ref, gr, gm)):
        for s, j in ((OWN, x), (OWN_A, links.xa), (OWN_B, links.xb)):
            dst[z, y, :, s * d_loc:(s + 2) * d_loc] = src[:, part_of(j, 2 * d_loc)]
        mine[dp] = src[:, part_of(dp, d_loc)]

    def each(group, *steps):
        for name, phase in steps:
            for unit in group:
                getattr(unit, name)(phase)

    row_half = SECTIONS * d_loc // 2
    x_rows = [Rows(links, xr, 0, row_half, True), Rows(links, xr, row_half, row_half, False)]
    g_rows = [Rows(links, gr, 0, row_half, True), Rows(links, gr, row_half, row_half, False)]

    def dp_half(h):
        return pl.ds(h * (N_DP // 2), N_DP // 2)

    def xc_first(p, h):
        return xc_ref.at[:, p, y] if h is None else xc_ref.at[dp_half(h), p, y]

    def xc_second(p, h):
        return xc_ref.at[:, :, p] if h is None else xc_ref.at[dp_half(h), :, p]

    def gc_first(p, h):
        return gc_ref.at[:, z, p] if h is None else gc_ref.at[dp_half(h), z, p]

    def gc_second(p, h):
        return gc_ref.at[:, p] if h is None else gc_ref.at[dp_half(h), p]

    gather_end(lent[0])
    each(x_rows, ("start", 0))
    gather_end(lent[1])
    each(x_rows, ("forward", 0), ("end", 0), ("start", 1))
    each(g_rows, ("start", 0))
    each(x_rows, ("forward", 1))
    links.put_all()
    gate.forward()
    each(g_rows, ("forward", 0), ("end", 0), ("start", 1))
    each(x_rows, ("end", 1))

    accs = (acc_g.at[pl.ds(0, rows)], acc_g.at[pl.ds(rows, rows)], acc_u.at[pl.ds(0, rows)])
    tile = min(TILE, ffh)
    n_tile = ffh // tile

    def take(ref, s, n):
        return ref[:, :, :, s * d_loc:(s + n) * d_loc].reshape(rows, n * d_loc)

    def product(src, s, n, w, first, t, down_side):
        if down_side:
            return dot(take(src, s, n), w[t, first * d_loc:(first + n) * d_loc], NT)
        return dot(take(src, s, n), w[first * d_loc:(first + n) * d_loc, t], NN)

    def lend_sums(k, src, wa, wb, down_side):
        def body(i):
            t = part_of(i, tile)
            q_out[k, 0, :, t] = product(src, TOK_B, 4, wa, 0, t, down_side)
            q_out[k, 1, :, t] = product(src, TOK_A, 4, wb, 0, t, down_side)
        loop(n_tile, body)
        return [links.send(q_out.at[k, 0], q_in.at[k, 0], "b"), links.send(q_out.at[k, 1], q_in.at[k, 1], "a")]

    def own_sums(k, src, wa, wb, down_side):
        def body(i):
            t = part_of(i, tile)
            accs[k][:, t] = product(src, OWN, 4, wa, 0, t, down_side)
            accs[k][:, part_of(i + n_tile, tile)] = (product(src, OWN, 2, wb, 0, t, down_side)
                                                     + product(src, OWN_B, 2, wb, 2, t, down_side))
        loop(n_tile, body)

    gate.near()
    qa = lend_sums(0, xr, wga, wgb, False)
    up.forward()
    up.near()
    qb = lend_sums(1, xr, wua, wub, False)
    for copies in spreads:
        gather_end(copies)
    links.put(xm, xc_first(z, None))
    links.put(gm, gc_first(y, None))
    each(g_rows, ("forward", 1))
    cx = gather_start(links, xm, xc_first, "z", z)
    cg = gather_start(links, gm, gc_first, "y", y)
    own_sums(0, xr, wga, wgb, False)
    own_sums(1, xr, wua, wub, False)
    down.forward()
    each(g_rows, ("end", 1))
    down.near()
    qg = lend_sums(2, gr, wda, wdb, True)
    cx = gather_forward(links, cx, xc_first, "z", z)
    cg = gather_forward(links, cg, gc_first, "y", y)
    own_sums(2, gr, wda, wdb, True)
    links.put_all()

    step_rows = 16

    def gate_loop(body):
        def step(i):
            r = part_of(i, step_rows)
            own = part_of(dp * (rows // step_rows) + i, step_rows)
            for h in (0, 1):
                cols = pl.ds(h * ffh, ffh)
                body(own, cols, lambda k: accs[k][r, cols] + q_in[k, h, r])
        loop(rows // step_rows, step)

    def hidden_body(own, cols, value):
        a = value(0)
        ha[own, cols] = (a * jax.nn.sigmoid(a) * value(1)).astype(bf16)

    gather_end(qa)
    gather_end(qb)
    gate_loop(hidden_body)
    mine = part_of(dp, rows)

    def row_slot(ref):
        def slot(j, h):
            if h is None:
                return ref.at[part_of(j, rows)]
            return ref.at[part_of(2 * j + h, rows // 2)]
        return slot

    hid = DpGather(links, ha.at[mine], row_slot(ha))
    gather_end(cx)
    cx = gather_start(links, xc_second(y, None), xc_second, "y", y)
    gather_end(cg)
    cg = gather_start(links, gc_second(z, None), gc_second, "z", z)

    def grad_body(own, cols, value):
        a, g = value(0), value(2)
        s = jax.nn.sigmoid(a)
        daa[own, cols] = (g * value(1) * (s * (1.0 + a * (1.0 - s)))).astype(bf16)
        dba[own, cols] = (g * (a * s)).astype(bf16)

    gather_end(qg)
    gate_loop(grad_body)
    dgate = DpGather(links, daa.at[mine], row_slot(daa))
    dup = DpGather(links, dba.at[mine], row_slot(dba))

    cx = gather_forward(links, cx, xc_second, "y", y)
    cg = gather_forward(links, cg, gc_second, "z", z)

    def clear(*refs):
        for ref in refs:
            n, step = ref.shape[0], min(16, ref.shape[0])

            def body(i):
                ref[part_of(i, step)] = jnp.zeros((step, ref.shape[1]), jnp.float32)
            loop(n // step, body)

    clear(acc_g, acc_u, acc_d)

    def block_of(s):
        p = s // 2
        return 2 * ((x + p + p // 2 - 2 * (p // 3)) % RING) + (core + s) % 2

    d_tile = min(TILE, d_loc)
    n_d = d_loc // d_tile
    ff_tile = min(TILE, ff)
    n_ff = ff // ff_tile
    low, high = pl.ds(0, ffh), pl.ds(ffh, ffh)
    torus = (RING, RING, tok)

    def y_blocks(lo, n):
        def body(i):
            s = lo + i // n_d
            r, t = part_of(block_of(s), rows), part_of(i % n_d, d_tile)
            w = part_of(core * n_d + i % n_d, d_tile)
            y_part[s, :, :, :, t] = (dot(ha[r, low], wda[:, w], NN) + dot(ha[r, high], wdb[:, w], NN)).reshape(
                torus + (d_tile,))
        loop(n * n_d, body)

    def gx_blocks(lo, n):
        def body(i):
            s = lo + i // n_d
            r, t = part_of(block_of(s), rows), part_of(i % n_d, d_tile)
            w = part_of(core * n_d + i % n_d, d_tile)
            gx_part[s, :, :, :, t] = (dot(daa[r, low], wga[w], NT) + dot(daa[r, high], wgb[w], NT)
                                      + dot(dba[r, low], wua[w], NT) + dot(dba[r, high], wub[w], NT)).reshape(
                torus + (d_tile,))
        loop(n * n_d, body)

    def cols_of(ref, j):
        return ref[:, :, :, part_of(j, d_loc)].reshape(rows, d_loc)

    def add_wd(lo, n):
        def body(i):
            j, t = block_of(lo + i // n_ff), part_of(i % n_ff, ff_tile)
            acc_d[t] += dot(ha[part_of(j, rows), t], cols_of(gr, j), TN)
        loop(n * n_ff, body)

    def add_wup(acc, src, lo, n):
        def body(i):
            j, t = block_of(lo + i // n_ff), part_of(i % n_ff, ff_tile)
            acc[pl.ds(0, d_loc), t] += dot(cols_of(xr, j), src[part_of(j, rows), t], TN)
        loop(n * n_ff, body)

    n_buf = 8
    groups = ((0,), (1,)), ((2, 3), (4, 5)), ((6,), (7,))

    def units(part, k):
        bufs = [scat_bufs[(6 * k + u) * n_buf:(6 * k + u + 1) * n_buf] for u in range(6)]
        return [[Scatter(links, part, pair[i], i == 0, bufs[2 * n + i]) for i in (0, 1)]
                for n, pair in enumerate(groups)]

    y_own, y_near, y_far = units(y_part, 0)
    g_own, g_near, g_far = units(gx_part, 1)
    returns = []

    def finish(group, part, resid, stage, out):
        for unit in group:
            unit.end(1)
            for s in unit.slots:
                j = block_of(s)
                piece = (resid[j].astype(jnp.float32) + part[s, z, y]).astype(bf16)
                if s == 0:
                    out[:, part_of(dp, d_loc)] = piece
                else:
                    stage[s] = piece
        for unit in group:
            for s in unit.slots:
                if s:
                    returns.append(links.send(stage.at[s], out.at[:, part_of(dp, d_loc)], "block", block_of(s)))

    for gathered in (hid, dgate, dup):
        gathered.own()
    y_blocks(0, 2)
    each(y_own, ("start", 0))
    each(y_own, ("forward", 0))
    hid.forward()
    hid.near()
    y_blocks(2, 4)
    each(y_near, ("start", 0))
    gather_end(cx)
    gather_end(cg)
    row_sends = [copy for rows_of in x_rows + g_rows for copy in rows_of.sent]
    for copy in row_sends:
        copy.wait_send()
    links.sent = [c for c in links.sent if not any(c is r for r in row_sends)]
    for j in range(N_DP):
        links.put(xc_ref.at[j], xr.at[:, :, :, pl.ds(j * d_loc, d_loc)])
        links.put(gc_ref.at[j], gr.at[:, :, :, pl.ds(j * d_loc, d_loc)])
    gx_blocks(0, 2)
    each(g_own, ("start", 0))
    dgate.forward()
    links.put_all()
    add_wd(0, 6)
    each(y_near, ("forward", 0))
    dgate.near()
    add_wup(acc_g, daa, 0, 6)
    each(y_near, ("end", 0), ("start", 1))
    each(y_own, ("end", 0), ("start", 1))
    dup.forward()
    each(g_own, ("forward", 0))
    each(y_near, ("forward", 1))
    dup.near()
    gx_blocks(2, 4)
    each(g_near, ("start", 0))
    hid.far()
    add_wup(acc_u, dba, 0, 6)
    hid.near()
    each(g_own, ("end", 0), ("start", 1))
    y_blocks(6, 2)
    each(y_far, ("start", 0))
    each(g_near, ("forward", 0))
    finish(y_near, y_part, xm, y_stage, y_ref)
    each(y_own, ("forward", 1))
    add_wd(6, 2)
    each(g_own, ("forward", 1))
    dgate.far()
    each(y_far, ("forward", 0))
    dgate.near()
    dup.far()
    dup.near()
    gx_blocks(6, 2)
    each(g_far, ("start", 0))
    add_wup(acc_g, daa, 6, 2)
    each(y_far, ("end", 0), ("start", 1))
    finish(y_own, y_part, xm, y_stage, y_ref)
    each(g_far, ("forward", 0))
    each(y_far, ("forward", 1))
    each(g_near, ("end", 0), ("start", 1))
    each(g_far, ("end", 0), ("start", 1))
    finish(y_far, y_part, xm, y_stage, y_ref)
    each(g_near, ("forward", 1))
    each(g_far, ("forward", 1))
    finish(g_own, gx_part, gm, gx_stage, gx_ref)
    finish(g_near, gx_part, gm, gx_stage, gx_ref)
    finish(g_far, gx_part, gm, gx_stage, gx_ref)
    add_wup(acc_u, dba, 6, 2)
    gather_end(returns)
    links.sent_all()
    links.put_all()


VMEM_LIMIT = 56 * 1024 * 1024


def copy_kernel(*refs):
    n = (len(refs) - 1) // 2
    ins, outs, sem = refs[:n], refs[n:2 * n], refs[-1]
    copies = [pltpu.make_async_copy(ins[k], outs[k], sem.at[k]) for k in range(n)]
    for copy in copies:
        copy.start()
    for copy in copies:
        copy.wait()


def solution(mesh):
    vmem = pl.BlockSpec(memory_space=VMEM)
    hbm = pl.BlockSpec(memory_space=pl.ANY)

    def local_step(x_loc, wg_loc, wu_loc, wd_loc, gy_loc):
        tok, d = x_loc.shape
        d_loc, ff = wg_loc.shape
        ffh = ff // 2
        bf16, f32 = x_loc.dtype, jnp.float32
        sds = jax.ShapeDtypeStruct
        n_sem = 288
        rows = RING * RING * tok
        spread = sds((N_DP, RING, RING, tok, d_loc), bf16)
        assert d_loc == 2 * rows
        whole = pltpu.VMEM((N_DP * rows, ff), bf16)
        mine = pltpu.VMEM((N_DP, tok, d_loc), bf16)
        scat = []
        for n in (1, 1, 2, 2, 1, 1):
            for half in ((n, 2, tok, d_loc), (n, tok, d_loc // 2)):
                scat += [pltpu.VMEM(half, f32)] * 2 + [pltpu.VMEM((2,) + half, f32)] * 2
        results = [sds((tok, d), bf16), sds((tok, d), bf16), sds((d_loc, ff), f32), sds((d_loc, ff), f32),
                   sds((ff, d_loc), f32)]
        outs = pl.pallas_call(
            mlp_kernel,
            out_shape=[VMEM(r.shape, r.dtype) for r in results] + [spread, spread],
            in_specs=[vmem] * 2 + [hbm] * 3,
            out_specs=[vmem] * 5 + [hbm] * 2,
            scratch_shapes=[pltpu.VMEM((4 * d_loc, ffh), bf16)] * 4 + [pltpu.VMEM((ffh, 4 * d_loc), bf16)] * 2
            + [pltpu.VMEM((RING, RING, tok, SECTIONS * d_loc), bf16)] * 2 + [mine] * 2
            + [pltpu.VMEM((3, 2, rows, ffh), f32)] * 2 + [whole] * 3
            + [pltpu.VMEM((N_DP, RING, RING, tok, d_loc), f32)] * 2 + [mine] * 2 + scat * 2
            + [pltpu.SemaphoreType.DMA((n_sem,)), pltpu.SemaphoreType.DMA((n_sem,)), pltpu.SemaphoreType.DMA((32,))],
            compiler_params=pltpu.CompilerParams(collective_id=0, has_side_effects=True, vmem_limit_bytes=VMEM_LIMIT),
            name="mlp",
        )(x_loc, gy_loc, wg_loc, wu_loc, wd_loc)[:5]
        return pl.pallas_call(
            copy_kernel,
            out_shape=results,
            in_specs=[vmem] * 5,
            out_specs=[hbm] * 5,
            scratch_shapes=[pltpu.SemaphoreType.DMA((5,))],
            compiler_params=pltpu.CompilerParams(vmem_limit_bytes=16 * 1024 * 1024),
            name="results",
        )(*outs)

    row_spec = P(("dp", "tp"), None)
    up_spec = P("dp", "tp")
    down_spec = P("tp", "dp")
    return jax.shard_map(local_step, mesh=mesh,
                         in_specs=(row_spec, up_spec, up_spec, down_spec, row_spec),
                         out_specs=(row_spec, row_spec, up_spec, up_spec, down_spec),
                         check_vma=False)
```
